8 devices in a mesh: dp: 1 (over z), dcp: 8 (over y, x, core).
Axes of the slice: x: 2, y: 2, z: 1, core: 2. Of those that a mesh axis runs over, the one named last changes fastest.
Arguments:
- q_abs: bfloat16 [128, 128, 576], P('dp', 'dcp')
- latent_cache: bfloat16 [128, 4, 8, 256, 576], P('dp', None, 'dcp')
- ctx_len: int32 [128], P('dp')
Outputs:
- output: bfloat16 [128, 128, 512], P(('dp', 'dcp'))
All inputs are finite; a program needn't handle non-finite values.
Results may differ from the reference program's by a relative error of at most 0.00644688.
Values are sent between devices in bfloat16 or wider.
A program may use at most 1 GiB of HBM per device.

```python
import math
import jax
import jax.numpy as jnp
from jax import lax

BATCH_SIZE = 128
NUM_HEADS = 128
LATENT_DIM = 512
ROPE_DIM = 64
NOPE_DIM = 128
PAGES_DEV = 4
GROUP_SIZE = 8
PAGE_LEN = 256

WIDTH = LATENT_DIM + ROPE_DIM
SEQ_LEN = PAGES_DEV * GROUP_SIZE * PAGE_LEN


def setup_inputs(seed: int = 0, part: int = 0) -> dict:
    part_key = jax.random.fold_in(jax.random.key(seed), part)
    key_query, key_cache, key_len = jax.random.split(part_key, 3)
    qk_dim = NOPE_DIM + ROPE_DIM
    cache_rope = 1.4
    query_latent = math.sqrt(0.95 * qk_dim / LATENT_DIM)
    query_rope = math.sqrt(0.95 * qk_dim / ROPE_DIM) / cache_rope
    is_latent = jnp.arange(WIDTH) < LATENT_DIM
    query_scale = jnp.where(is_latent, query_latent, query_rope)
    cache_scale = jnp.where(is_latent, 1.0, cache_rope)
    queries = jax.random.normal(key_query, (BATCH_SIZE, NUM_HEADS, WIDTH), jnp.float32) * query_scale
    cache_vals = jax.random.normal(key_cache, (BATCH_SIZE, PAGES_DEV, GROUP_SIZE, PAGE_LEN, WIDTH), jnp.float32) * cache_scale
    len_drop = jax.random.randint(key_len, (BATCH_SIZE,), 0, SEQ_LEN // 2)
    lengths = jnp.where(jnp.arange(BATCH_SIZE) == 0, SEQ_LEN, SEQ_LEN - len_drop)
    return {'q_abs': queries.astype(jnp.bfloat16), 'latent_cache': cache_vals.astype(jnp.bfloat16), 'ctx_len': lengths.astype(jnp.int32)}


def reference(q_abs, latent_cache, ctx_len):
    inv_scale = (NOPE_DIM + ROPE_DIM) ** -0.5
    q_float = q_abs.astype(jnp.float32)
    per_device = jnp.moveaxis(latent_cache, 2, 0)
    page_base = jnp.arange(PAGES_DEV)[:, None] * (GROUP_SIZE * PAGE_LEN) + jnp.arange(PAGE_LEN)[None, :]

    def one_device(carry_in):
        dev_index, cache_blk = carry_in
        cache_float = cache_blk.astype(jnp.float32)
        scores = jnp.einsum('bhw,bjtw->bhjt', q_float, cache_float) * inv_scale
        positions = page_base + dev_index * PAGE_LEN
        is_valid = positions[None, :, :] < ctx_len[:, None, None]
        scores = jnp.where(is_valid[:, None, :, :], scores, -1e30)
        row_max = jnp.max(scores, axis=(2, 3))
        weights_exp = jnp.exp(scores - row_max[:, :, None, None])
        denom_sum = jnp.sum(weights_exp, axis=(2, 3))
        weights_low = weights_exp.astype(jnp.bfloat16).astype(jnp.float32)
        pv_sum = jnp.einsum('bhjt,bjtc->bhc', weights_low, cache_float[..., :LATENT_DIM])
        part_out = (pv_sum / denom_sum[:, :, None]).astype(jnp.bfloat16)
        part_lse = row_max + jnp.log(denom_sum)
        return part_out, part_lse

    part_outs, part_lses = lax.map(one_device, (jnp.arange(GROUP_SIZE), per_device))
    total_lse = jax.nn.logsumexp(part_lses, axis=0)
    merge_weights = jnp.exp(part_lses - total_lse[None])
    merged = jnp.sum(merge_weights[..., None] * part_outs.astype(jnp.float32), axis=0)
    return merged.astype(jnp.bfloat16)
```

```python
import functools

import jax
import jax.numpy as jnp
from jax import lax
from jax.experimental import pallas as pl
from jax.experimental.pallas import tpu as pltpu
from jax.sharding import PartitionSpec as P

ROPE_DIM = 64
QK_DIM = 192
MESH = pl.DeviceIdType.MESH
NEG = -1e30

CACHE_SLOTS = 4
RING = 4
MERGE_LAG = 1
FINAL_LAG = 3


def _kernel(dims, len_ref, q_ref, cache_ref, out_ref, q_all, cbuf, o_tx, lse_acc, lse_tx, rx, rx_lse, m_tx, m_lse, rxm, rxm_lse,
            w_rows, o_stage, q_sem, c_sem, ag_send, ag_recv, o_send, o_recv, l_send, l_recv, m_send, m_recv, ml_send, ml_recv, out_sem):
    steps, group, heads, width, pages, page_len = dims
    latent = width - ROPE_DIM
    scale = QK_DIM ** -0.5
    me = lax.axis_index('dcp')
    core = me % 2
    x = (me // 2) % 2
    y = me // 4

    def dev(dx, dy, c):
        return ((y + dy) % 2 * 2 + (x + dx) % 2) * 2 + c

    n1x, n1y = core, 1 - core
    n2x, n2y = 1 - core, core
    n1 = dev(n1x, n1y, core)
    n2 = dev(n2x, n2y, core)
    partner = dev(0, 0, 1 - core)
    diag = dev(1, 1, core)

    owners = (
        dev(1, 1, 0), dev(1, 0, 0),
        dev(1, 1, 1), dev(0, 1, 1),
        dev(n2x, n2y, 1 - core), partner,
        dev(n1x, n1y, core), me,
    )
    targets = (dev(1, 0, 0), dev(0, 1, 1), partner)

    def to(device):
        return {'dcp': device}

    barrier = pltpu.get_barrier_semaphore()
    for other in range(1, group):
        pl.semaphore_signal(barrier, inc=1, device_id=to((me + other) % group), device_id_type=MESH)

    def q_load(u):
        return pltpu.make_async_copy(q_ref.at[:, u], q_all.at[u, :, me], q_sem.at[u])

    def c_load(i, r):
        slot = r % CACHE_SLOTS
        return pltpu.make_async_copy(cache_ref.at[owners[r] * steps + i, :, 0], cbuf.at[slot], c_sem.at[slot])

    def ag(u, kind):
        block = (me, me, me, n2, n2, n1, diag)[kind]
        target = (n2, n1, partner, n1, partner, partner, partner)[kind]
        return pltpu.make_async_remote_copy(
            src_ref=q_all.at[u, :, block], dst_ref=q_all.at[u, :, block],
            send_sem=ag_send.at[u, kind], recv_sem=ag_recv.at[u, kind],
            device_id=to(target), device_id_type=MESH)

    def ag_own(u):
        q_load(u).wait()
        for kind in range(3):
            ag(u, kind).start()

    def ag_forward(u):
        ag(u, 0).wait_recv()
        ag(u, 3).start()
        ag(u, 4).start()
        ag(u, 1).wait_recv()
        ag(u, 5).start()

    def ag_relay(u):
        ag(u, 3).wait_recv()
        ag(u, 6).start()

    def ag_ready(u):
        for kind in (2, 4, 5, 6):
            ag(u, kind).wait_recv()

    def o_copy(i, t):
        ring = i % RING
        dst = (0, 0, 2)[t]
        return pltpu.make_async_remote_copy(
            src_ref=o_tx.at[ring, t], dst_ref=rx.at[i, core if t < 2 else 2],
            send_sem=o_send.at[ring, t], recv_sem=o_recv.at[i, core if t < 2 else 2],
            device_id=to(targets[t]), device_id_type=MESH)

    def l_copy(i, t):
        ring = i % RING
        return pltpu.make_async_remote_copy(
            src_ref=lse_tx.at[ring], dst_ref=rx_lse.at[i, core if t < 2 else 2],
            send_sem=l_send.at[ring, t], recv_sem=l_recv.at[i, core if t < 2 else 2],
            device_id=to(targets[t]), device_id_type=MESH)

    def rx_wait(i, s):
        pltpu.make_async_remote_copy(
            src_ref=o_tx.at[0, 0], dst_ref=rx.at[i, s], send_sem=o_send.at[0, 0], recv_sem=o_recv.at[i, s],
            device_id=to(partner), device_id_type=MESH).wait_recv()
        pltpu.make_async_remote_copy(
            src_ref=lse_tx.at[0], dst_ref=rx_lse.at[i, s], send_sem=l_send.at[0, 0], recv_sem=l_recv.at[i, s],
            device_id=to(partner), device_id_type=MESH).wait_recv()

    def m_copy(i):
        ring = i % RING
        return pltpu.make_async_remote_copy(
            src_ref=m_tx.at[ring], dst_ref=rxm.at[i], send_sem=m_send.at[ring], recv_sem=m_recv.at[i],
            device_id=to(n1), device_id_type=MESH)

    def ml_copy(i):
        ring = i % RING
        return pltpu.make_async_remote_copy(
            src_ref=m_lse.at[ring], dst_ref=rxm_lse.at[i], send_sem=ml_send.at[ring], recv_sem=ml_recv.at[i],
            device_id=to(n1), device_id_type=MESH)

    def out_copy(i):
        return pltpu.make_async_copy(o_stage.at[i % 2], out_ref.at[i], out_sem.at[i % 2])

    lane = lax.broadcasted_iota(jnp.int32, (heads, 128), 1)
    col = lax.broadcasted_iota(jnp.int32, (1, page_len), 1)

    def attend(i, r):
        slot = r % CACHE_SLOTS
        c_load(i, r).wait()
        q = q_all[i, owners[r]].reshape(heads, width)
        length = len_ref[owners[r] * steps + i]
        scores = []
        for j in range(pages):
            s = lax.dot_general(q, cbuf[slot, j], (((1,), (0,)), ((), ())), preferred_element_type=jnp.float32) * scale
            first = (j * group + me) * page_len
            scores.append(jnp.where(col + first < length, s, NEG))
        row_max = functools.reduce(jnp.maximum, [jnp.max(s, axis=1, keepdims=True) for s in scores])
        total = jnp.zeros((heads, 1), jnp.float32)
        acc = jnp.zeros((heads, latent), jnp.float32)
        for j in range(pages):
            w = jnp.exp(scores[j] - row_max)
            total = total + jnp.sum(w, axis=1, keepdims=True)
            acc = acc + lax.dot_general(w.astype(jnp.bfloat16), cbuf[slot, j, :latent], (((1,), (1,)), ((), ())),
                                        preferred_element_type=jnp.float32)
        o_tx[i % RING, r // 2, r % 2] = (acc / total).astype(jnp.bfloat16)
        lse_acc[...] = jnp.where(lane == r, row_max + jnp.log(total), lse_acc[...])

    def weighted(rows, blocks):
        top = functools.reduce(jnp.maximum, rows)
        exps = [jnp.exp(v - top) for v in rows]
        total = functools.reduce(jnp.add, exps)
        lse = top + jnp.log(total)
        for n, v in enumerate(rows):
            w_rows[n:n + 1, :] = jnp.exp(v - lse)
        cols = w_rows[...].T
        acc = cols[:, 0:1] * blocks[0].astype(jnp.float32)
        for n in range(1, len(blocks)):
            acc = acc + cols[:, n:n + 1] * blocks[n].astype(jnp.float32)
        return lse, acc

    def pick(block, k):
        return jnp.where(core == 0, block[k:k + 1], block[2 + k:3 + k])

    def merge(i):
        ring = i % RING
        for s in range(3):
            rx_wait(i, s)
        rows = [lse_tx[ring][6:7], pick(rx_lse[i, 0], 0), pick(rx_lse[i, 1], 0), rx_lse[i, 2][4:5]]
        lse, acc = weighted(rows, [o_tx[ring, 3, 0], rx[i, 0, 0], rx[i, 1, 0], rx[i, 2, 0]])
        m_tx[ring] = acc
        m_lse[ring] = jnp.broadcast_to(lse, (8, heads))

    def final(i):
        ring = i % RING
        m_recv_wait(i)
        rows = [lse_tx[ring][7:8], pick(rx_lse[i, 0], 1), pick(rx_lse[i, 1], 1), rx_lse[i, 2][5:6], rxm_lse[i][0:1]]
        _, acc = weighted(rows, [o_tx[ring, 3, 1], rx[i, 0, 1], rx[i, 1, 1], rx[i, 2, 1], rxm[i]])
        o_stage[i % 2] = acc.astype(jnp.bfloat16)

    def m_recv_wait(i):
        m_copy(i).wait_recv()
        ml_copy(i).wait_recv()

    for r in range(CACHE_SLOTS - 1):
        c_load(0, r).start()

    @pl.loop(0, steps)
    def _(u):
        q_load(u).start()

    w_rows[...] = jnp.zeros_like(w_rows)
    lse_acc[...] = jnp.zeros_like(lse_acc)
    pl.semaphore_wait(barrier, group - 1)

    for u in range(4):
        ag_own(u)
    for u in range(2):
        ag_forward(u)
    for u in range(2):
        ag_relay(u)

    @pl.loop(0, steps + FINAL_LAG)
    def _(i):
        gathering = i < steps // 2 - 1

        @pl.when(i < steps)
        def _():
            @pl.when(i >= RING)
            def _():
                for t in range(3):
                    o_copy(i - RING, t).wait_send()
                    l_copy(i - RING, t).wait_send()

            ag_ready(i)
            for r in range(group):
                ahead = r + CACHE_SLOTS - 1
                if ahead < group:
                    c_load(i, ahead).start()
                else:
                    @pl.when(i + 1 < steps)
                    def _():
                        c_load(i + 1, ahead - group).start()
                attend(i, r)
                if r in (1, 3, 5):
                    o_copy(i, r // 2).start()
                if r in (0, 4):
                    @pl.when(i < steps // 2 - 2)
                    def _():
                        ag_own(2 * i + 4 + r // 4)
                if r in (2, 4):
                    @pl.when(gathering)
                    def _():
                        ag_forward(2 * i + 2 + r // 4)
                if r in (5, 7):
                    @pl.when(gathering)
                    def _():
                        ag_relay(2 * i + 2 + r // 6)
            lse_tx[i % RING] = lse_acc[...].T[0:8]
            for t in range(3):
                l_copy(i, t).start()

        @pl.when((i >= MERGE_LAG) & (i < steps + MERGE_LAG))
        def _():
            k = i - MERGE_LAG

            @pl.when(k >= RING)
            def _():
                m_copy(k - RING).wait_send()
                ml_copy(k - RING).wait_send()

            merge(k)
            m_copy(k).start()
            ml_copy(k).start()

        @pl.when(i >= FINAL_LAG)
        def _():
            k = i - FINAL_LAG

            @pl.when(k >= 2)
            def _():
                out_copy(k - 2).wait()

            final(k)
            out_copy(k).start()

    @pl.loop(steps - RING, steps)
    def _(i):
        for t in range(3):
            o_copy(i, t).wait_send()
            l_copy(i, t).wait_send()
        m_copy(i).wait_send()
        ml_copy(i).wait_send()

    @pl.loop(0, steps)
    def _(u):
        for kind in range(7):
            ag(u, kind).wait_send()

    for i in (steps - 2, steps - 1):
        out_copy(i).wait()


def solution(mesh):
    group = mesh.shape['dcp']

    def local_step(q_blk, cache_blk, len_blk):
        batch, own_heads, width = q_blk.shape
        pages, page_len = cache_blk.shape[1], cache_blk.shape[3]
        steps = batch // group
        heads = own_heads * group
        latent = width - ROPE_DIM
        bf16, f32 = jnp.bfloat16, jnp.float32
        dma = pltpu.SemaphoreType.DMA
        return pl.pallas_call(
            functools.partial(_kernel, (steps, group, heads, width, pages, page_len)),
            out_shape=jax.ShapeDtypeStruct((steps, heads, latent), bf16),
            in_specs=[pl.BlockSpec(memory_space=pltpu.SMEM), pl.BlockSpec(memory_space=pl.ANY), pl.BlockSpec(memory_space=pl.ANY)],
            out_specs=pl.BlockSpec(memory_space=pl.ANY),
            scratch_shapes=[
                pltpu.VMEM((steps, group, group, own_heads, width), bf16),
                pltpu.VMEM((CACHE_SLOTS, pages, width, page_len), bf16),
                pltpu.VMEM((RING, 4, 2, heads, latent), bf16),
                pltpu.VMEM((heads, 128), f32),
                pltpu.VMEM((RING, 8, heads), f32),
                pltpu.VMEM((steps, 3, 2, heads, latent), bf16),
                pltpu.VMEM((steps, 3, 8, heads), f32),
                pltpu.VMEM((RING, heads, latent), f32),
                pltpu.VMEM((RING, 8, heads), f32),
                pltpu.VMEM((steps, heads, latent), f32),
                pltpu.VMEM((steps, 8, heads), f32),
                pltpu.VMEM((128, heads), f32),
                pltpu.VMEM((2, heads, latent), bf16),
                dma((steps,)), dma((CACHE_SLOTS,)),
                dma((steps, 7)), dma((steps, 7)),
                dma((RING, 3)), dma((steps, 3)), dma((RING, 3)), dma((steps, 3)),
                dma((RING,)), dma((steps,)), dma((RING,)), dma((steps,)),
                dma((2,)),
            ],
            compiler_params=pltpu.CompilerParams(collective_id=0, has_side_effects=True, vmem_limit_bytes=66_000_000),
        )(len_blk, q_blk.reshape(group, steps, own_heads, width), jnp.swapaxes(cache_blk, 3, 4))

    return jax.shard_map(local_step, mesh=mesh, in_specs=(P('dp', 'dcp', None), P('dp', None, 'dcp', None, None), P('dp')),
                         out_specs=P(('dp', 'dcp'), None, None), check_vma=False)
```

```python
import functools

import jax
import jax.numpy as jnp
from jax import lax
from jax.experimental import pallas as pl
from jax.experimental.pallas import tpu as pltpu
from jax.sharding import PartitionSpec as P

ROPE_DIM = 64
QK_DIM = 192
MESH = pl.DeviceIdType.MESH
NEG = -1e30

CACHE_SLOTS = 4
RING = 4
LEAD = 1
FINAL_LAG = 1


def _kernel(dims, len_ref, q_ref, cache_ref, out_ref, q_all, cbuf, o_tx, lse_acc, lse_a, lse_b, rx_d, rx_f, rx_p, rx_la, rx_lb,
            m_tx, m_lse, rx_m, rx_ml, w_rows, o_stage, q_sem, c_sem, ag_send, ag_recv, d_send, d_recv, f_send, f_recv, p_send, p_recv,
            la_send, la_recv, lb_send, lb_recv, m_send, m_recv, ml_send, ml_recv, out_sem):
    steps, group, heads, latent, pages, page_len = dims
    scale = QK_DIM ** -0.5
    me = lax.axis_index('dcp')
    core = me % 2
    x = (me // 2) % 2
    y = me // 4

    def dev(dx, dy, c):
        return ((y + dy) % 2 * 2 + (x + dx) % 2) * 2 + c

    n1x, n1y = core, 1 - core
    n2x, n2y = 1 - core, core
    n1 = dev(n1x, n1y, core)
    n2 = dev(n2x, n2y, core)
    partner = dev(0, 0, 1 - core)
    diag = dev(1, 1, core)
    x0, y1 = dev(1, 0, 0), dev(0, 1, 1)

    OM, PM, D0, D1, F0, F1, PF, OF = range(8)
    owners = (
        dev(n1x, n1y, core),
        dev(n2x, n2y, 1 - core),
        dev(1, 1, 0), dev(1, 1, 1),
        x0, y1,
        partner, me,
    )

    def remote(src, dst, send, recv, device):
        return pltpu.make_async_remote_copy(src_ref=src, dst_ref=dst, send_sem=send, recv_sem=recv,
                                            device_id={'dcp': device}, device_id_type=MESH)

    barrier = pltpu.get_barrier_semaphore()
    for other in range(1, group):
        pl.semaphore_signal(barrier, inc=1, device_id={'dcp': (me + other) % group}, device_id_type=MESH)

    def q_load(u):
        return pltpu.make_async_copy(q_ref.at[u], q_all.at[u, :, me], q_sem.at[u])

    def row(it, p):
        return it if p in (D0, D1) else it - LEAD

    def valid(it, p):
        return it < steps if p in (D0, D1) else (it >= LEAD) & (it < steps + LEAD)

    def c_load(it, p):
        slot = p % CACHE_SLOTS
        return pltpu.make_async_copy(cache_ref.at[owners[p] * steps + row(it, p), :, 0], cbuf.at[slot], c_sem.at[slot])

    def out_copy(i):
        return pltpu.make_async_copy(o_stage.at[i % 2], out_ref.at[i], out_sem.at[i % 2])

    def ag(u, kind):
        block = (me, me, me, n2, n2, n1, diag)[kind]
        target = (n2, n1, partner, n1, partner, partner, partner)[kind]
        return remote(q_all.at[u, :, block], q_all.at[u, :, block], ag_send.at[u, kind], ag_recv.at[u, kind], target)

    def ag_own(u):
        q_load(u).wait()
        for kind in range(3):
            ag(u, kind).start()

    def ag_forward(u):
        ag(u, 0).wait_recv()
        ag(u, 3).start()
        ag(u, 4).start()
        ag(u, 1).wait_recv()
        ag(u, 5).start()

    def ag_relay(u):
        ag(u, 3).wait_recv()
        ag(u, 6).start()

    def ag_ready(u):
        for kind in (2, 4, 5, 6):
            ag(u, kind).wait_recv()

    def d_copy(it, t):
        ring = it % RING
        return remote(o_tx.at[ring, D0 + t], rx_d.at[it, core], d_send.at[ring, t], d_recv.at[it, core], (x0, y1)[t])

    def f_copy(it, t):
        ring, i = it % RING, it - LEAD
        return remote(o_tx.at[ring, F0 + t], rx_f.at[i, core], f_send.at[ring, t], f_recv.at[i, core], (x0, y1)[t])

    def p_copy(it, t):
        ring, i = it % RING, it - LEAD
        return remote(o_tx.at[ring, (PM, PF)[t]], rx_p.at[i, t], p_send.at[ring, t], p_recv.at[i, t], partner)

    def la_copy(it):
        ring, i = it % RING, it - LEAD
        return remote(lse_a.at[ring], rx_la.at[i], la_send.at[ring], la_recv.at[i], partner)

    def lb_copy(it, t):
        ring = it % RING
        s = core if t < 2 else 2
        return remote(lse_b.at[ring], rx_lb.at[it, s], lb_send.at[ring, t], lb_recv.at[it, s], (x0, y1, partner)[t])

    def m_copy(it):
        ring, i = it % RING, it - LEAD
        return remote(m_tx.at[ring], rx_m.at[i], m_send.at[ring], m_recv.at[i], n1)

    def ml_copy(it):
        ring, i = it % RING, it - LEAD
        return remote(m_lse.at[ring], rx_ml.at[i], ml_send.at[ring], ml_recv.at[i], n1)

    def sent(it):
        @pl.when(it < steps)
        def _():
            for t in range(2):
                d_copy(it, t).wait_send()

        @pl.when((it >= LEAD) & (it < steps + LEAD))
        def _():
            for t in range(2):
                f_copy(it, t).wait_send()
                p_copy(it, t).wait_send()
            la_copy(it).wait_send()
            m_copy(it).wait_send()
            ml_copy(it).wait_send()

        for t in range(3):
            lb_copy(it, t).wait_send()

    def landed(dst, recv, src):
        remote(src, dst, d_send.at[0, 0], recv, partner).wait_recv()

    lane = lax.broadcasted_iota(jnp.int32, (heads, 128), 1)
    col = lax.broadcasted_iota(jnp.int32, (1, page_len), 1)

    def attend(it, p, lse_row):
        slot = p % CACHE_SLOTS
        u, k = row(it, p), owners[p]
        c_load(it, p).wait()
        q = q_all[u, k].reshape(heads, latent)
        pair = q_all[u, group, :, :, pl.ds(pl.multiple_of(k // 2 * 128, 128), 128)].reshape(heads, 128)
        rope = jnp.where(k % 2 == 0, pair[:, :ROPE_DIM], pair[:, ROPE_DIM:])
        length = len_ref[k * steps + u]
        scores = []
        for j in range(pages):
            s = jnp.dot(q, cbuf[slot, j, :latent], preferred_element_type=jnp.float32)
            s = (s + jnp.dot(rope, cbuf[slot, j, latent:], preferred_element_type=jnp.float32)) * scale
            first = (j * group + me) * page_len
            scores.append(jnp.where(col + first < length, s, NEG))
        row_max = functools.reduce(jnp.maximum, [jnp.max(s, axis=1, keepdims=True) for s in scores])
        total = jnp.zeros((heads, 1), jnp.float32)
        acc = jnp.zeros((heads, latent), jnp.float32)
        for j in range(pages):
            w = jnp.exp(scores[j] - row_max)
            total = total + jnp.sum(w, axis=1, keepdims=True)
            acc = acc + lax.dot_general(w.astype(jnp.bfloat16), cbuf[slot, j, :latent], (((1,), (1,)), ((), ())),
                                        preferred_element_type=jnp.float32)
        o_tx[it % RING, p] = (acc / total).astype(jnp.bfloat16)
        lse_acc[...] = jnp.where(lane == lse_row, row_max + jnp.log(total), lse_acc[...])

    def weighted(rows, blocks):
        top = functools.reduce(jnp.maximum, rows)
        total = functools.reduce(jnp.add, [jnp.exp(v - top) for v in rows])
        lse = top + jnp.log(total)
        for n, v in enumerate(rows):
            w_rows[n:n + 1, :] = jnp.exp(v - lse)
        cols = w_rows[...].T
        acc = cols[:, 0:1] * blocks[0].astype(jnp.float32)
        for n in range(1, len(blocks)):
            acc = acc + cols[:, n:n + 1] * blocks[n].astype(jnp.float32)
        return lse, acc

    def pick(block, k):
        return jnp.where(core == 0, block[k:k + 1], block[k + 1:k + 2])

    def merge(it):
        ring, i = it % RING, it - LEAD
        for s in range(2):
            landed(rx_d.at[i, s], d_recv.at[i, s], o_tx.at[0, 0])
            landed(rx_lb.at[i, s], lb_recv.at[i, s], lse_b.at[0])
        p_copy(it, 0).wait_recv()
        la_copy(it).wait_recv()
        rows = [lse_a[ring][0:1], pick(rx_lb[i, 0], 0), pick(rx_lb[i, 1], 0), rx_la[i][1:2]]
        lse, acc = weighted(rows, [o_tx[ring, OM], rx_d[i, 0], rx_d[i, 1], rx_p[i, 0]])
        m_tx[ring] = acc
        m_lse[ring] = jnp.broadcast_to(lse, (8, heads))

    def final(it):
        ring, i = it % RING, it - LEAD
        for s in range(2):
            landed(rx_f.at[i, s], f_recv.at[i, s], o_tx.at[0, 0])

            @pl.when(it >= steps)
            def _():
                landed(rx_lb.at[it, s], lb_recv.at[it, s], lse_b.at[0])

        p_copy(it, 1).wait_recv()
        lb_copy(it, 2).wait_recv()
        m_copy(it).wait_recv()
        ml_copy(it).wait_recv()
        rows = [lse_b[ring][5:6], pick(rx_lb[it, 0], 2), pick(rx_lb[it, 1], 2), rx_lb[it, 2][4:5], rx_ml[i][0:1]]
        _, acc = weighted(rows, [o_tx[ring, OF], rx_f[i, 0], rx_f[i, 1], rx_p[i, 1], rx_m[i]])
        o_stage[i % 2] = acc.astype(jnp.bfloat16)

    @pl.loop(0, steps)
    def _(u):
        q_load(u).start()

    for p in range(CACHE_SLOTS - 1):
        if p in (D0, D1):
            c_load(0, p).start()

    w_rows[...] = jnp.zeros_like(w_rows)
    lse_acc[...] = jnp.zeros_like(lse_acc)
    pl.semaphore_wait(barrier, group - 1)

    ag_own(0)
    ag_own(1)
    ag_forward(0)
    ag_own(2)
    ag_forward(1)
    ag_relay(0)
    ag_own(3)
    ag_relay(1)

    def gather(it, phase):
        if phase == 0:
            @pl.when(it < steps // 2 - 2)
            def _():
                ag_own(2 * it + 4)
                ag_own(2 * it + 5)
        elif phase == 1:
            @pl.when(it < steps // 2 - 1)
            def _():
                ag_forward(2 * it + 2)
                ag_forward(2 * it + 3)
        else:
            @pl.when((it >= 1) & (it < steps // 2))
            def _():
                ag_relay(2 * it)
                ag_relay(2 * it + 1)

    @pl.loop(0, steps + LEAD + FINAL_LAG)
    def _(it):
        @pl.when(it >= RING)
        def _():
            sent(it - RING)

        @pl.when(it < steps)
        def _():
            ag_ready(it)

        gather(it, 0)
        for p in range(group):
            ahead = p + CACHE_SLOTS - 1
            nxt = it + ahead // group

            @pl.when(valid(nxt, ahead % group))
            def _():
                c_load(nxt, ahead % group).start()

            @pl.when(valid(it, p))
            def _():
                attend(it, p, (0, 1, 0, 1, 2, 3, 4, 5)[p])
                if p == PM:
                    lse_a[it % RING] = lse_acc[...].T[0:8]
                    p_copy(it, 0).start()
                    la_copy(it).start()
                elif p in (D0, D1):
                    d_copy(it, p - D0).start()
                elif p in (F0, F1):
                    f_copy(it, p - F0).start()
                elif p == PF:
                    p_copy(it, 1).start()
                if p == F1:
                    merge(it)
                    m_copy(it).start()
                    ml_copy(it).start()

            if p == D1:
                gather(it, 1)
            if p == F1:
                gather(it, 2)

        @pl.when(it < steps + LEAD)
        def _():
            lse_b[it % RING] = lse_acc[...].T[0:8]
            for t in range(3):
                lb_copy(it, t).start()

        @pl.when(it >= LEAD + FINAL_LAG)
        def _():
            k = it - FINAL_LAG

            @pl.when(k >= LEAD + 2)
            def _():
                out_copy(k - LEAD - 2).wait()

            final(k)
            out_copy(k - LEAD).start()

    @pl.loop(steps + LEAD + FINAL_LAG - RING, steps + LEAD)
    def _(it):
        sent(it)

    for it in range(LEAD):
        landed(rx_lb.at[it, 2], lb_recv.at[it, 2], lse_b.at[0])

    @pl.loop(0, steps)
    def _(u):
        for kind in range(7):
            ag(u, kind).wait_send()

    for i in (steps - 2, steps - 1):
        out_copy(i).wait()


def solution(mesh):
    group = mesh.shape['dcp']

    def local_step(q_blk, cache_blk, len_blk):
        batch, own_heads, width = q_blk.shape
        pages, page_len = cache_blk.shape[1], cache_blk.shape[3]
        steps = batch // group
        heads = own_heads * group
        latent = width - ROPE_DIM
        bf16, f32 = jnp.bfloat16, jnp.float32
        dma = pltpu.SemaphoreType.DMA
        q_steps = q_blk.reshape(group, steps, own_heads, width)
        q_latent = jnp.transpose(q_steps[..., :latent], (1, 0, 2, 3))
        q_rope = jnp.transpose(q_steps[..., latent:], (1, 2, 0, 3)).reshape(steps, 1, own_heads, group * ROPE_DIM)
        q_blocks = jnp.concatenate([q_latent, q_rope], axis=1)
        return pl.pallas_call(
            functools.partial(_kernel, (steps, group, heads, latent, pages, page_len)),
            out_shape=jax.ShapeDtypeStruct((steps, heads, latent), bf16),
            in_specs=[pl.BlockSpec(memory_space=pltpu.SMEM), pl.BlockSpec(memory_space=pl.ANY), pl.BlockSpec(memory_space=pl.ANY)],
            out_specs=pl.BlockSpec(memory_space=pl.ANY),
            scratch_shapes=[
                pltpu.VMEM((steps, group + 1, group, own_heads, latent), bf16),
                pltpu.VMEM((CACHE_SLOTS, pages, width, page_len), bf16),
                pltpu.VMEM((RING, group, heads, latent), bf16),
                pltpu.VMEM((heads, 128), f32),
                pltpu.VMEM((RING, 8, heads), f32),
                pltpu.VMEM((RING, 8, heads), f32),
                pltpu.VMEM((steps, 2, heads, latent), bf16),
                pltpu.VMEM((steps, 2, heads, latent), bf16),
                pltpu.VMEM((steps, 2, heads, latent), bf16),
                pltpu.VMEM((steps, 8, heads), f32),
                pltpu.VMEM((steps + LEAD, 3, 8, heads), f32),
                pltpu.VMEM((RING, heads, latent), f32),
                pltpu.VMEM((RING, 8, heads), f32),
                pltpu.VMEM((steps, heads, latent), f32),
                pltpu.VMEM((steps, 8, heads), f32),
                pltpu.VMEM((128, heads), f32),
                pltpu.VMEM((2, heads, latent), bf16),
                dma((steps,)), dma((CACHE_SLOTS,)),
                dma((steps, 7)), dma((steps, 7)),
                dma((RING, 2)), dma((steps, 2)),
                dma((RING, 2)), dma((steps, 2)),
                dma((RING, 2)), dma((steps, 2)),
                dma((RING,)), dma((steps,)),
                dma((RING, 3)), dma((steps + LEAD, 3)),
                dma((RING,)), dma((steps,)), dma((RING,)), dma((steps,)),
                dma((2,)),
            ],
            compiler_params=pltpu.CompilerParams(collective_id=0, has_side_effects=True, vmem_limit_bytes=66_000_000),
        )(len_blk, q_blocks, jnp.swapaxes(cache_blk, 3, 4))

    return jax.shard_map(local_step, mesh=mesh, in_specs=(P('dp', 'dcp', None), P('dp', None, 'dcp', None, None), P('dp')),
                         out_specs=P(('dp', 'dcp'), None, None), check_vma=False)
```

```python
import functools

import jax
import jax.numpy as jnp
from jax import lax
from jax.experimental import pallas as pl
from jax.experimental.pallas import tpu as pltpu
from jax.sharding import PartitionSpec as P

ROPE_DIM = 64
QK_DIM = 192
MESH = pl.DeviceIdType.MESH
NEG = -1e30

CACHE_SLOTS = 4
RING = 4
LEAD = 1
FINAL_LAG = 1


def _kernel(dims, len_hbm, q_hbm, cache_ref, out_ref, len_ref, q_own, q_all, cbuf, o_tx, lse_acc, lse_a, lse_b, rx_d, rx_f, rx_p, rx_la, rx_lb,
            m_tx, m_lse, rx_m, rx_ml, w_rows, o_stage, len_sem, q_sem, c_sem, ag_send, ag_recv, d_send, d_recv, f_send, f_recv, p_send, p_recv,
            la_send, la_recv, lb_send, lb_recv, m_send, m_recv, ml_send, ml_recv, out_sem):
    steps, group, heads, latent, pages, page_len = dims
    scale = QK_DIM ** -0.5
    me = lax.axis_index('dcp')
    core = me % 2
    x = (me // 2) % 2
    y = me // 4

    def dev(dx, dy, c):
        return ((y + dy) % 2 * 2 + (x + dx) % 2) * 2 + c

    n1x, n1y = core, 1 - core
    n2x, n2y = 1 - core, core
    n1 = dev(n1x, n1y, core)
    n2 = dev(n2x, n2y, core)
    partner = dev(0, 0, 1 - core)
    diag = dev(1, 1, core)
    x0, y1 = dev(1, 0, 0), dev(0, 1, 1)

    OM, PM, D0, D1, F0, F1, PF, OF = range(8)
    owners = (
        dev(n1x, n1y, core),
        dev(n2x, n2y, 1 - core),
        dev(1, 1, 0), dev(1, 1, 1),
        x0, y1,
        partner, me,
    )

    def remote(src, dst, send, recv, device):
        return pltpu.make_async_remote_copy(src_ref=src, dst_ref=dst, send_sem=send, recv_sem=recv,
                                            device_id={'dcp': device}, device_id_type=MESH)

    barrier = pltpu.get_barrier_semaphore()
    for other in range(1, group):
        pl.semaphore_signal(barrier, inc=1, device_id={'dcp': (me + other) % group}, device_id_type=MESH)

    def len_load():
        return pltpu.make_async_copy(len_hbm, len_ref, len_sem)

    def q_load():
        return pltpu.make_async_copy(q_hbm, q_own, q_sem)

    def row(it, p):
        return it if p in (D0, D1) else it - LEAD

    def valid(it, p):
        return it < steps if p in (D0, D1) else (it >= LEAD) & (it < steps + LEAD)

    def c_load(it, p):
        slot = p % CACHE_SLOTS
        return pltpu.make_async_copy(cache_ref.at[owners[p] * steps + row(it, p), :, 0], cbuf.at[slot], c_sem.at[slot])

    def out_copy(i):
        return pltpu.make_async_copy(o_stage.at[i % 2], out_ref.at[i], out_sem.at[i % 2])

    def ag(u, kind):
        block = (me, me, me, n2, n2, n1, diag)[kind]
        target = (n2, n1, partner, n1, partner, partner, partner)[kind]
        return remote(q_all.at[u, :, block], q_all.at[u, :, block], ag_send.at[u, kind], ag_recv.at[u, kind], target)

    wide_row = lax.broadcasted_iota(jnp.int32, (heads, steps * group), 0)
    wide_lane = lax.broadcasted_iota(jnp.int32, (heads, steps * group), 1)
    own_heads = heads // group
    own_head = wide_row % own_heads

    def q_build(u):
        chosen = wide_lane == wide_row // own_heads * steps + u
        acc = None
        for h in range(0, own_heads, 2):
            one_hot = jnp.concatenate([jnp.where(chosen & (own_head == g), 1.0, 0.0) for g in (h, h + 1)], axis=1)
            pair = jnp.concatenate([q_own[h], q_own[h + 1]], axis=1)
            term = lax.dot_general(one_hot.astype(jnp.bfloat16), pair, (((1,), (1,)), ((), ())), preferred_element_type=jnp.float32)
            acc = term if acc is None else acc + term
        q_all[u, 0:group, me] = acc[:, :latent].astype(jnp.bfloat16).reshape(group, own_heads, latent)
        ropes = [acc[k * own_heads:(k + 1) * own_heads, latent:] for k in range(group)]
        q_all[u, group, me] = jnp.concatenate(ropes, axis=1).astype(jnp.bfloat16)

    def ag_own(u):
        q_build(u)
        for kind in range(3):
            ag(u, kind).start()

    def ag_forward(u):
        ag(u, 0).wait_recv()
        ag(u, 3).start()
        ag(u, 4).start()
        ag(u, 1).wait_recv()
        ag(u, 5).start()

    def ag_relay(u):
        ag(u, 3).wait_recv()
        ag(u, 6).start()

    def ag_ready(u):
        for kind in (2, 4, 5, 6):
            ag(u, kind).wait_recv()

    def d_copy(it, t):
        ring = it % RING
        return remote(o_tx.at[ring, D0 + t], rx_d.at[it, core], d_send.at[ring, t], d_recv.at[it, core], (x0, y1)[t])

    def f_copy(it, t):
        ring, i = it % RING, it - LEAD
        return remote(o_tx.at[ring, F0 + t], rx_f.at[i, core], f_send.at[ring, t], f_recv.at[i, core], (x0, y1)[t])

    def p_copy(it, t):
        ring, i = it % RING, it - LEAD
        return remote(o_tx.at[ring, (PM, PF)[t]], rx_p.at[i, t], p_send.at[ring, t], p_recv.at[i, t], partner)

    def la_copy(it):
        ring, i = it % RING, it - LEAD
        return remote(lse_a.at[ring], rx_la.at[i], la_send.at[ring], la_recv.at[i], partner)

    def lb_copy(it, t):
        ring = it % RING
        s = core if t < 2 else 2
        return remote(lse_b.at[ring, t], rx_lb.at[it, s], lb_send.at[ring, t], lb_recv.at[it, s], (x0, y1, partner)[t])

    def m_copy(it):
        ring, i = it % RING, it - LEAD
        return remote(m_tx.at[ring], rx_m.at[i], m_send.at[ring], m_recv.at[i], n1)

    def ml_copy(it):
        ring, i = it % RING, it - LEAD
        return remote(m_lse.at[ring], rx_ml.at[i], ml_send.at[ring], ml_recv.at[i], n1)

    def sent(it):
        @pl.when(it < steps)
        def _():
            for t in range(2):
                d_copy(it, t).wait_send()

        @pl.when((it >= LEAD) & (it < steps + LEAD))
        def _():
            for t in range(2):
                f_copy(it, t).wait_send()
                p_copy(it, t).wait_send()
            la_copy(it).wait_send()
            m_copy(it).wait_send()
            ml_copy(it).wait_send()

        for t in range(3):
            lb_copy(it, t).wait_send()

    def landed(dst, recv, src):
        remote(src, dst, d_send.at[0, 0], recv, partner).wait_recv()

    lane = lax.broadcasted_iota(jnp.int32, (heads, 128), 1)
    col = lax.broadcasted_iota(jnp.int32, (1, page_len), 1)

    def attend(it, p, lse_row):
        slot = p % CACHE_SLOTS
        u, k = row(it, p), owners[p]
        c_load(it, p).wait()
        q = q_all[u, k].reshape(heads, latent)
        pair = q_all[u, group, :, :, pl.ds(pl.multiple_of(k // 2 * 128, 128), 128)].reshape(heads, 128)
        rope = jnp.where(k % 2 == 0, pair[:, :ROPE_DIM], pair[:, ROPE_DIM:])
        length = len_ref[k * steps + u]
        scores = []
        for j in range(pages):
            s = jnp.dot(q, cbuf[slot, j, :latent], preferred_element_type=jnp.float32)
            s = (s + jnp.dot(rope, cbuf[slot, j, latent:], preferred_element_type=jnp.float32)) * scale
            first = (j * group + me) * page_len
            scores.append(jnp.where(col + first < length, s, NEG))
        row_max = functools.reduce(jnp.maximum, [jnp.max(s, axis=1, keepdims=True) for s in scores])
        total = jnp.zeros((heads, 1), jnp.float32)
        acc = jnp.zeros((heads, latent), jnp.float32)
        for j in range(pages):
            w = jnp.exp(scores[j] - row_max)
            total = total + jnp.sum(w, axis=1, keepdims=True)
            acc = acc + lax.dot_general(w.astype(jnp.bfloat16), cbuf[slot, j, :latent], (((1,), (1,)), ((), ())),
                                        preferred_element_type=jnp.float32)
        o_tx[it % RING, p] = (acc / total).astype(jnp.bfloat16)
        lse_acc[...] = jnp.where(lane == lse_row, row_max + jnp.log(total), lse_acc[...])

    def weighted(rows, blocks):
        top = functools.reduce(jnp.maximum, rows)
        total = functools.reduce(jnp.add, [jnp.exp(v - top) for v in rows])
        lse = top + jnp.log(total)
        for n, v in enumerate(rows):
            w_rows[n:n + 1, :] = jnp.exp(v - lse)
        cols = w_rows[...].T
        acc = cols[:, 0:1] * blocks[0].astype(jnp.float32)
        for n in range(1, len(blocks)):
            acc = acc + cols[:, n:n + 1] * blocks[n].astype(jnp.float32)
        return lse, acc

    def merge(it):
        ring, i = it % RING, it - LEAD
        for s in range(2):
            landed(rx_d.at[i, s], d_recv.at[i, s], o_tx.at[0, 0])
            landed(rx_lb.at[i, s], lb_recv.at[i, s], lse_b.at[0, 0])
        p_copy(it, 0).wait_recv()
        la_copy(it).wait_recv()
        rows = [lse_a[ring][0:1], rx_lb[i, 0][0:1], rx_lb[i, 1][0:1], rx_la[i][1:2]]
        lse, acc = weighted(rows, [o_tx[ring, OM], rx_d[i, 0], rx_d[i, 1], rx_p[i, 0]])
        m_tx[ring] = acc
        m_lse[ring] = lse

    def final(it):
        ring, i = it % RING, it - LEAD
        for s in range(2):
            landed(rx_f.at[i, s], f_recv.at[i, s], o_tx.at[0, 0])

            @pl.when(it >= steps)
            def _():
                landed(rx_lb.at[it, s], lb_recv.at[it, s], lse_b.at[0, 0])

        p_copy(it, 1).wait_recv()
        lb_copy(it, 2).wait_recv()
        m_copy(it).wait_recv()
        ml_copy(it).wait_recv()
        rows = [lse_b[ring, 2][1:2], rx_lb[it, 0][1:2], rx_lb[it, 1][1:2], rx_lb[it, 2][0:1], rx_ml[i]]
        _, acc = weighted(rows, [o_tx[ring, OF], rx_f[i, 0], rx_f[i, 1], rx_p[i, 1], rx_m[i]])
        o_stage[i % 2] = acc.astype(jnp.bfloat16)

    q_load().start()
    len_load().start()
    for p in range(CACHE_SLOTS - 1):
        if p in (D0, D1):
            c_load(0, p).start()

    w_rows[...] = jnp.zeros_like(w_rows)
    lse_acc[...] = jnp.zeros_like(lse_acc)
    q_load().wait()
    pl.semaphore_wait(barrier, group - 1)

    ag_own(0)
    ag_own(1)
    ag_forward(0)
    ag_own(2)
    ag_forward(1)
    ag_relay(0)
    ag_own(3)
    ag_relay(1)
    len_load().wait()

    def gather(it, phase):
        if phase == 0:
            @pl.when(it < steps // 2 - 2)
            def _():
                ag_own(2 * it + 4)
                ag_own(2 * it + 5)
        elif phase == 1:
            @pl.when(it < steps // 2 - 1)
            def _():
                ag_forward(2 * it + 2)
                ag_forward(2 * it + 3)
        else:
            @pl.when((it >= 1) & (it < steps // 2))
            def _():
                ag_relay(2 * it)
                ag_relay(2 * it + 1)

    @pl.loop(0, steps + LEAD + FINAL_LAG)
    def _(it):
        @pl.when(it >= RING)
        def _():
            sent(it - RING)

        @pl.when(it < steps)
        def _():
            ag_ready(it)

        gather(it, 0)
        for p in range(group):
            ahead = p + CACHE_SLOTS - 1
            nxt = it + ahead // group

            @pl.when(valid(nxt, ahead % group))
            def _():
                c_load(nxt, ahead % group).start()

            @pl.when(valid(it, p))
            def _():
                attend(it, p, (6, 7, 0, 2, 1, 3, 4, 5)[p])
                if p == PM:
                    lse_a[it % RING] = lse_acc[...].T[6:8]
                    p_copy(it, 0).start()
                    la_copy(it).start()
                elif p in (D0, D1):
                    d_copy(it, p - D0).start()
                elif p in (F0, F1):
                    f_copy(it, p - F0).start()
                elif p == PF:
                    p_copy(it, 1).start()
                if p == F1:
                    merge(it)
                    m_copy(it).start()
                    ml_copy(it).start()

            if p == D1:
                gather(it, 1)
            if p == F1:
                gather(it, 2)

        @pl.when(it < steps + LEAD)
        def _():
            rows = lse_acc[...].T
            for t in range(3):
                lse_b[it % RING, t] = rows[2 * t:2 * t + 2]
            for t in range(3):
                lb_copy(it, t).start()

        @pl.when(it >= LEAD + FINAL_LAG)
        def _():
            k = it - FINAL_LAG

            @pl.when(k >= LEAD + 2)
            def _():
                out_copy(k - LEAD - 2).wait()

            final(k)
            out_copy(k - LEAD).start()

    @pl.loop(steps + LEAD + FINAL_LAG - RING, steps + LEAD)
    def _(it):
        sent(it)

    for it in range(LEAD):
        landed(rx_lb.at[it, 2], lb_recv.at[it, 2], lse_b.at[0, 0])

    @pl.loop(0, steps)
    def _(u):
        for kind in range(7):
            ag(u, kind).wait_send()

    for i in (steps - 2, steps - 1):
        out_copy(i).wait()


def solution(mesh):
    group = mesh.shape['dcp']

    def local_step(q_blk, cache_blk, len_blk):
        batch, own_heads, width = q_blk.shape
        pages, page_len = cache_blk.shape[1], cache_blk.shape[3]
        steps = batch // group
        heads = own_heads * group
        latent = width - ROPE_DIM
        bf16, f32 = jnp.bfloat16, jnp.float32
        dma = pltpu.SemaphoreType.DMA
        return pl.pallas_call(
            functools.partial(_kernel, (steps, group, heads, latent, pages, page_len)),
            out_shape=jax.ShapeDtypeStruct((steps, heads, latent), bf16),
            in_specs=[pl.BlockSpec(memory_space=pl.ANY)] * 3,
            out_specs=pl.BlockSpec(memory_space=pl.ANY),
            scratch_shapes=[
                pltpu.SMEM((batch,), jnp.int32),
                pltpu.VMEM((own_heads, width, batch), bf16),
                pltpu.VMEM((steps, group + 1, group, own_heads, latent), bf16),
                pltpu.VMEM((CACHE_SLOTS, pages, width, page_len), bf16),
                pltpu.VMEM((RING, group, heads, latent), bf16),
                pltpu.VMEM((heads, 128), f32),
                pltpu.VMEM((RING, 2, heads), f32),
                pltpu.VMEM((RING, 3, 2, heads), f32),
                pltpu.VMEM((steps, 2, heads, latent), bf16),
                pltpu.VMEM((steps, 2, heads, latent), bf16),
                pltpu.VMEM((steps, 2, heads, latent), bf16),
                pltpu.VMEM((steps, 2, heads), f32),
                pltpu.VMEM((steps + LEAD, 3, 2, heads), f32),
                pltpu.VMEM((RING, heads, latent), f32),
                pltpu.VMEM((RING, 1, heads), f32),
                pltpu.VMEM((steps, heads, latent), f32),
                pltpu.VMEM((steps, 1, heads), f32),
                pltpu.VMEM((128, heads), f32),
                pltpu.VMEM((2, heads, latent), bf16),
                dma, dma, dma((CACHE_SLOTS,)),
                dma((steps, 7)), dma((steps, 7)),
                dma((RING, 2)), dma((steps, 2)),
                dma((RING, 2)), dma((steps, 2)),
                dma((RING, 2)), dma((steps, 2)),
                dma((RING,)), dma((steps,)),
                dma((RING, 3)), dma((steps + LEAD, 3)),
                dma((RING,)), dma((steps,)), dma((RING,)), dma((steps,)),
                dma((2,)),
            ],
            compiler_params=pltpu.CompilerParams(collective_id=0, has_side_effects=True, vmem_limit_bytes=66_000_000),
        )(len_blk, jnp.transpose(q_blk, (1, 2, 0)), jnp.swapaxes(cache_blk, 3, 4))

    return jax.shard_map(local_step, mesh=mesh, in_specs=(P('dp', 'dcp', None), P('dp', None, 'dcp', None, None), P('dp')),
                         out_specs=P(('dp', 'dcp'), None, None), check_vma=False)
```

```python
import functools

import jax
import jax.numpy as jnp
from jax import lax
from jax.experimental import pallas as pl
from jax.experimental.pallas import tpu as pltpu
from jax.sharding import PartitionSpec as P

ROPE_DIM = 64
QK_DIM = 192
MESH = pl.DeviceIdType.MESH
NEG = -1e30

CACHE_SLOTS = 4
RING = 4
AG_RING = 8
LEAD = 1
FINAL_LAG = 1


def _kernel(dims, len_hbm, q_hbm, cache_ref, out_ref, len_ref, q_own, q_all, cbuf, o_tx, lse_acc, lse_a, lse_b, rx_d, rx_f, rx_la, rx_lb,
            m_tx, m_lse, rx_m, rx_ml, w_rows, o_stage, len_sem, q_sem, c_sem, out_sem, ag_send, ag_recv, ag_part,
            d_send, f_send, la_send, lb_send, m_send, ml_send, d_recv, f_recv, la_recv, lb_recv, m_recv, ml_recv):
    steps, group, heads, latent, pages, page_len = dims
    scale = QK_DIM ** -0.5
    me = lax.axis_index('dcp')
    core = me % 2
    x = (me // 2) % 2
    y = me // 4

    def dev(dx, dy, c):
        return ((y + dy) % 2 * 2 + (x + dx) % 2) * 2 + c

    n1x, n1y = core, 1 - core
    n2x, n2y = 1 - core, core
    n1 = dev(n1x, n1y, core)
    n2 = dev(n2x, n2y, core)
    partner = dev(0, 0, 1 - core)
    diag = dev(1, 1, core)
    x0, y1 = dev(1, 0, 0), dev(0, 1, 1)

    OM, PM, D0, D1, F0, F1, PF, OF = range(8)
    owners = (
        dev(n1x, n1y, core),
        dev(n2x, n2y, 1 - core),
        dev(1, 1, 0), dev(1, 1, 1),
        x0, y1,
        partner, me,
    )

    def remote(src, dst, send, recv, device):
        return pltpu.make_async_remote_copy(src_ref=src, dst_ref=dst, send_sem=send, recv_sem=recv,
                                            device_id={'dcp': device}, device_id_type=MESH)

    barrier = pltpu.get_barrier_semaphore()
    peers = (n1, n2, partner)
    for peer in peers:
        pl.semaphore_signal(barrier, inc=1, device_id={'dcp': peer}, device_id_type=MESH)

    def len_load():
        return pltpu.make_async_copy(len_hbm, len_ref, len_sem)

    def q_load():
        return pltpu.make_async_copy(q_hbm, q_own, q_sem)

    def row(it, p):
        return it if p in (D0, D1) else it - LEAD

    def valid(it, p):
        return it < steps if p in (D0, D1) else (it >= LEAD) & (it < steps + LEAD)

    def c_load(it, p):
        slot = p % CACHE_SLOTS
        return pltpu.make_async_copy(cache_ref.at[owners[p] * steps + row(it, p), :, 0], cbuf.at[slot], c_sem.at[slot])

    def out_copy(i):
        return pltpu.make_async_copy(o_stage.at[i % 2], out_ref.at[i], out_sem.at[i % 2])

    def ag(u, kind):
        block = (me, me, me, n2, n2, n1, diag)[kind]
        target = (n2, n1, partner, n1, partner, partner, partner)[kind]
        recv = ag_part.at[u] if kind in (2, 4, 5, 6) else ag_recv.at[u % AG_RING, (0, 1, None, 2)[kind]]
        return remote(q_all.at[u, :, block], q_all.at[u, :, block], ag_send.at[kind], recv, target)

    wide_row = lax.broadcasted_iota(jnp.int32, (heads, steps * group), 0)
    wide_lane = lax.broadcasted_iota(jnp.int32, (heads, steps * group), 1)
    own_heads = heads // group
    own_head = wide_row % own_heads

    def q_build(u):
        chosen = wide_lane == wide_row // own_heads * steps + u
        acc = None
        for h in range(0, own_heads, 2):
            one_hot = jnp.concatenate([jnp.where(chosen & (own_head == g), 1.0, 0.0) for g in (h, h + 1)], axis=1)
            pair = jnp.concatenate([q_own[h], q_own[h + 1]], axis=1)
            term = lax.dot_general(one_hot.astype(jnp.bfloat16), pair, (((1,), (1,)), ((), ())), preferred_element_type=jnp.float32)
            acc = term if acc is None else acc + term
        q_all[u, 0:group, me] = acc[:, :latent].astype(jnp.bfloat16).reshape(group, own_heads, latent)
        ropes = [acc[k * own_heads:(k + 1) * own_heads, latent:] for k in range(group)]
        q_all[u, group, me] = jnp.concatenate(ropes, axis=1).astype(jnp.bfloat16)

    def ag_own(u):
        q_build(u)
        ag_send_own(u)

    def ag_send_own(u):
        for kind in range(3):
            ag(u, kind).start()

    def ag_forward(u):
        ag(u, 0).wait_recv()
        ag(u, 3).start()
        ag(u, 4).start()
        ag(u, 1).wait_recv()
        ag(u, 5).start()

    def ag_relay(u):
        ag(u, 3).wait_recv()
        ag(u, 6).start()

    def ag_ready(u):
        pltpu.make_async_copy(q_all.at[u, :, 0:4], q_all.at[u, :, 0:4], ag_part.at[u]).wait()

    def d_copy(it, t):
        ring = it % RING
        return remote(o_tx.at[ring, D0 + t], rx_d.at[it, core], d_send.at[ring], d_recv.at[ring], (x0, y1)[t])

    def pm_copy(it):
        ring, i = it % RING, it - LEAD
        return remote(o_tx.at[ring, PM], rx_d.at[i, 2], f_send.at[ring], d_recv.at[i % RING], partner)

    def f_copy(it, t):
        ring, i = it % RING, it - LEAD
        return remote(o_tx.at[ring, (F0, F1, PF)[t]], rx_f.at[i, core if t < 2 else 2], f_send.at[ring], f_recv.at[ring],
                      (x0, y1, partner)[t])

    def la_copy(it):
        ring, i = it % RING, it - LEAD
        return remote(lse_a.at[ring], rx_la.at[i], la_send.at[ring], la_recv.at[ring], partner)

    def lb_copy(it, t):
        ring = it % RING
        return remote(lse_b.at[ring, t], rx_lb.at[it, core if t < 2 else 2], lb_send.at[ring], lb_recv.at[ring], (x0, y1, partner)[t])

    def m_copy(it):
        ring, i = it % RING, it - LEAD
        return remote(m_tx.at[ring], rx_m.at[i], m_send.at[ring], m_recv.at[ring], n1)

    def ml_copy(it):
        ring, i = it % RING, it - LEAD
        return remote(m_lse.at[ring], rx_ml.at[i], ml_send.at[ring], ml_recv.at[ring], n1)

    def wait_bytes(ref, sem):
        pltpu.make_async_copy(ref, ref, sem).wait()

    def sent(it):
        ring = it % RING

        @pl.when(it < steps)
        def _():
            wait_bytes(o_tx.at[ring, 0:2], d_send.at[ring])

        @pl.when((it >= LEAD) & (it < steps + LEAD))
        def _():
            wait_bytes(o_tx.at[ring, 0:4], f_send.at[ring])
            wait_bytes(lse_a.at[ring], la_send.at[ring])
            wait_bytes(m_tx.at[ring], m_send.at[ring])
            wait_bytes(m_lse.at[ring], ml_send.at[ring])

        wait_bytes(lse_b.at[ring], lb_send.at[ring])

    lane = lax.broadcasted_iota(jnp.int32, (heads, 128), 1)
    col = lax.broadcasted_iota(jnp.int32, (1, page_len), 1)

    def attend(it, p, lse_row):
        slot = p % CACHE_SLOTS
        u, k = row(it, p), owners[p]
        c_load(it, p).wait()
        q = q_all[u, k].reshape(heads, latent)
        pair = q_all[u, group, :, :, pl.ds(pl.multiple_of(k // 2 * 128, 128), 128)].reshape(heads, 128)
        rope = jnp.where(k % 2 == 0, pair[:, :ROPE_DIM], pair[:, ROPE_DIM:])
        length = len_ref[k * steps + u]
        scores = []
        for j in range(pages):
            s = jnp.dot(q, cbuf[slot, j, :latent], preferred_element_type=jnp.float32)
            s = (s + jnp.dot(rope, cbuf[slot, j, latent:], preferred_element_type=jnp.float32)) * scale
            first = (j * group + me) * page_len
            scores.append(jnp.where(col + first < length, s, NEG))
        row_max = functools.reduce(jnp.maximum, [jnp.max(s, axis=1, keepdims=True) for s in scores])
        total = jnp.zeros((heads, 1), jnp.float32)
        acc = jnp.zeros((heads, latent), jnp.float32)
        for j in range(pages):
            w = jnp.exp(scores[j] - row_max)
            total = total + jnp.sum(w, axis=1, keepdims=True)
            acc = acc + lax.dot_general(w.astype(jnp.bfloat16), cbuf[slot, j, :latent], (((1,), (1,)), ((), ())),
                                        preferred_element_type=jnp.float32)
        o_tx[it % RING, p] = (acc / total).astype(jnp.bfloat16)
        lse_acc[...] = jnp.where(lane == lse_row, row_max + jnp.log(total), lse_acc[...])

    def weighted(rows, blocks):
        top = functools.reduce(jnp.maximum, rows)
        total = functools.reduce(jnp.add, [jnp.exp(v - top) for v in rows])
        lse = top + jnp.log(total)
        for n, v in enumerate(rows):
            w_rows[n:n + 1, :] = jnp.exp(v - lse)
        cols = w_rows[...].T
        acc = cols[:, 0:1] * blocks[0].astype(jnp.float32)
        for n in range(1, len(blocks)):
            acc = acc + cols[:, n:n + 1] * blocks[n].astype(jnp.float32)
        return lse, acc

    def merge(it):
        ring, i = it % RING, it - LEAD
        wait_bytes(rx_d.at[i], d_recv.at[i % RING])
        wait_bytes(rx_lb.at[i], lb_recv.at[i % RING])
        wait_bytes(rx_la.at[i], la_recv.at[ring])
        rows = [lse_a[ring][0:1], rx_lb[i, 0][0:1], rx_lb[i, 1][0:1], rx_la[i][1:2]]
        lse, acc = weighted(rows, [o_tx[ring, OM], rx_d[i, 0], rx_d[i, 1], rx_d[i, 2]])
        m_tx[ring] = acc
        m_lse[ring] = lse

    def final(it):
        ring, i = it % RING, it - LEAD
        wait_bytes(rx_f.at[i], f_recv.at[ring])

        @pl.when(it >= steps)
        def _():
            wait_bytes(rx_lb.at[it], lb_recv.at[ring])

        wait_bytes(rx_m.at[i], m_recv.at[ring])
        wait_bytes(rx_ml.at[i], ml_recv.at[ring])
        rows = [lse_b[ring, 2][1:2], rx_lb[it, 0][1:2], rx_lb[it, 1][1:2], rx_lb[it, 2][0:1], rx_ml[i]]
        _, acc = weighted(rows, [o_tx[ring, OF], rx_f[i, 0], rx_f[i, 1], rx_f[i, 2], rx_m[i]])
        o_stage[i % 2] = acc.astype(jnp.bfloat16)

    q_load().start()
    len_load().start()
    for p in range(CACHE_SLOTS - 1):
        if p in (D0, D1):
            c_load(0, p).start()

    w_rows[...] = jnp.zeros_like(w_rows)
    lse_acc[...] = jnp.zeros_like(lse_acc)
    q_load().wait()
    q_build(0)
    pl.semaphore_wait(barrier, len(peers))

    ag_send_own(0)
    ag_own(1)
    ag_forward(0)
    ag_own(2)
    ag_forward(1)
    ag_relay(0)
    ag_own(3)
    ag_relay(1)
    len_load().wait()

    def gather(it, phase):
        if phase == 0:
            @pl.when(it < steps // 2 - 2)
            def _():
                ag_own(2 * it + 4)
                ag_own(2 * it + 5)
        elif phase == 1:
            @pl.when(it < steps // 2 - 1)
            def _():
                ag_forward(2 * it + 2)
                ag_forward(2 * it + 3)
        else:
            @pl.when((it >= 1) & (it < steps // 2))
            def _():
                ag_relay(2 * it)
                ag_relay(2 * it + 1)

    @pl.loop(0, steps + LEAD + FINAL_LAG)
    def _(it):
        @pl.when(it >= RING)
        def _():
            sent(it - RING)

        @pl.when(it < steps)
        def _():
            ag_ready(it)

        gather(it, 0)
        for p in range(group):
            ahead = p + CACHE_SLOTS - 1
            nxt = it + ahead // group

            @pl.when(valid(nxt, ahead % group))
            def _():
                c_load(nxt, ahead % group).start()

            @pl.when(valid(it, p))
            def _():
                attend(it, p, (6, 7, 0, 2, 1, 3, 4, 5)[p])
                if p == PM:
                    lse_a[it % RING] = lse_acc[...].T[6:8]
                    pm_copy(it).start()
                    la_copy(it).start()
                elif p in (D0, D1):
                    d_copy(it, p - D0).start()
                elif p in (F0, F1):
                    f_copy(it, p - F0).start()
                elif p == PF:
                    f_copy(it, 2).start()
                if p == F1:
                    merge(it)
                    m_copy(it).start()
                    ml_copy(it).start()

            if p == D1:
                gather(it, 1)
            if p == F1:
                gather(it, 2)

        @pl.when(it < steps + LEAD)
        def _():
            rows = lse_acc[...].T
            for t in range(3):
                lse_b[it % RING, t] = rows[2 * t:2 * t + 2]
            for t in range(3):
                lb_copy(it, t).start()

        @pl.when(it >= LEAD + FINAL_LAG)
        def _():
            k = it - FINAL_LAG

            @pl.when(k >= LEAD + 2)
            def _():
                out_copy(k - LEAD - 2).wait()

            final(k)
            out_copy(k - LEAD).start()

    @pl.loop(steps + LEAD + FINAL_LAG - RING, steps + LEAD)
    def _(it):
        sent(it)

    for kind in range(7):
        wait_bytes(q_all.at[:, :, kind], ag_send.at[kind])

    for i in (steps - 2, steps - 1):
        out_copy(i).wait()


def solution(mesh):
    group = mesh.shape['dcp']

    def local_step(q_blk, cache_blk, len_blk):
        batch, own_heads, width = q_blk.shape
        pages, page_len = cache_blk.shape[1], cache_blk.shape[3]
        steps = batch // group
        heads = own_heads * group
        latent = width - ROPE_DIM
        bf16, f32 = jnp.bfloat16, jnp.float32
        dma = pltpu.SemaphoreType.DMA
        return pl.pallas_call(
            functools.partial(_kernel, (steps, group, heads, latent, pages, page_len)),
            out_shape=jax.ShapeDtypeStruct((steps, heads, latent), bf16),
            in_specs=[pl.BlockSpec(memory_space=pl.ANY)] * 3,
            out_specs=pl.BlockSpec(memory_space=pl.ANY),
            scratch_shapes=[
                pltpu.SMEM((batch,), jnp.int32),
                pltpu.VMEM((own_heads, width, batch), bf16),
                pltpu.VMEM((steps, group + 1, group, own_heads, latent), bf16),
                pltpu.VMEM((CACHE_SLOTS, pages, width, page_len), bf16),
                pltpu.VMEM((RING, group, heads, latent), bf16),
                pltpu.VMEM((heads, 128), f32),
                pltpu.VMEM((RING, 2, heads), f32),
                pltpu.VMEM((RING, 3, 2, heads), f32),
                pltpu.VMEM((steps, 3, heads, latent), bf16),
                pltpu.VMEM((steps, 3, heads, latent), bf16),
                pltpu.VMEM((steps, 2, heads), f32),
                pltpu.VMEM((steps + LEAD, 3, 2, heads), f32),
                pltpu.VMEM((RING, heads, latent), f32),
                pltpu.VMEM((RING, 1, heads), f32),
                pltpu.VMEM((steps, heads, latent), f32),
                pltpu.VMEM((steps, 1, heads), f32),
                pltpu.VMEM((128, heads), f32),
                pltpu.VMEM((2, heads, latent), bf16),
                dma, dma, dma((CACHE_SLOTS,)), dma((2,)),
                dma((7,)), dma((AG_RING, 3)), dma((steps,)),
                *[dma((RING,))] * 12,
            ],
            compiler_params=pltpu.CompilerParams(collective_id=0, has_side_effects=True, vmem_limit_bytes=66_000_000),
        )(len_blk, jnp.transpose(q_blk, (1, 2, 0)), jnp.swapaxes(cache_blk, 3, 4))

    return jax.shard_map(local_step, mesh=mesh, in_specs=(P('dp', 'dcp', None), P('dp', None, 'dcp', None, None), P('dp')),
                         out_specs=P(('dp', 'dcp'), None, None), check_vma=False)
```

```python
import functools

import jax
import jax.numpy as jnp
from jax import lax
from jax.experimental import pallas as pl
from jax.experimental.pallas import tpu as pltpu
from jax.sharding import PartitionSpec as P

ROPE_DIM = 64
QK_DIM = 192
MESH = pl.DeviceIdType.MESH
NEG = -1e30

CACHE_SLOTS = 4
RING = 4
AG_RING = 8
RX_RING = 8
LEAD = 2
FINAL_LAG = 2


def _kernel(dims, len_hbm, q_hbm, cache_ref, out_ref, len_ref, q_own, q_all, cbuf, o_tx, lse_acc, lse_a, lse_b, rx_d, rx_f, rx_la, rx_lb,
            m_tx, m_lse, rx_m, rx_ml, w_rows, o_stage, len_sem, q_sem, c_sem, out_sem, ag_send, ag_recv, ag_part,
            d_send, f_send, la_send, lb_send, m_send, ml_send, d_recv, f_recv, la_recv, lb_recv, m_recv, ml_recv):
    steps, group, heads, latent, pages, page_len = dims
    scale = QK_DIM ** -0.5
    me = lax.axis_index('dcp')
    core = me % 2
    x = (me // 2) % 2
    y = me // 4

    def dev(dx, dy, c):
        return ((y + dy) % 2 * 2 + (x + dx) % 2) * 2 + c

    n1x, n1y = core, 1 - core
    n2x, n2y = 1 - core, core
    n1 = dev(n1x, n1y, core)
    n2 = dev(n2x, n2y, core)
    partner = dev(0, 0, 1 - core)
    diag = dev(1, 1, core)
    x0, y1 = dev(1, 0, 0), dev(0, 1, 1)

    OM, PM, D0, D1, F0, F1, PF, OF = range(8)
    owners = (
        dev(n1x, n1y, core),
        dev(n2x, n2y, 1 - core),
        dev(1, 1, 0), dev(1, 1, 1),
        x0, y1,
        partner, me,
    )

    def remote(src, dst, send, recv, device):
        return pltpu.make_async_remote_copy(src_ref=src, dst_ref=dst, send_sem=send, recv_sem=recv,
                                            device_id={'dcp': device}, device_id_type=MESH)

    barrier = pltpu.get_barrier_semaphore()
    peers = (n1, n2, partner)
    for peer in peers:
        pl.semaphore_signal(barrier, inc=1, device_id={'dcp': peer}, device_id_type=MESH)

    def len_load():
        return pltpu.make_async_copy(len_hbm, len_ref, len_sem)

    def q_load():
        return pltpu.make_async_copy(q_hbm, q_own, q_sem)

    def row(it, p):
        return it if p in (D0, D1) else it - LEAD

    def valid(it, p):
        return it < steps if p in (D0, D1) else (it >= LEAD) & (it < steps + LEAD)

    def c_load(it, p):
        slot = p % CACHE_SLOTS
        return pltpu.make_async_copy(cache_ref.at[owners[p] * steps + row(it, p), :, 0], cbuf.at[slot], c_sem.at[slot])

    def out_copy(i):
        return pltpu.make_async_copy(o_stage.at[i % 2], out_ref.at[i], out_sem.at[i % 2])

    def ag(u, kind):
        block = (me, me, me, n2, n2, n1, diag)[kind]
        target = (n2, n1, partner, n1, partner, partner, partner)[kind]
        recv = ag_part.at[u] if kind in (2, 4, 5, 6) else ag_recv.at[u % AG_RING, (0, 1, None, 2)[kind]]
        return remote(q_all.at[u, :, block], q_all.at[u, :, block], ag_send.at[kind], recv, target)

    wide_row = lax.broadcasted_iota(jnp.int32, (heads, steps * group), 0)
    wide_lane = lax.broadcasted_iota(jnp.int32, (heads, steps * group), 1)
    own_heads = heads // group
    own_head = wide_row % own_heads

    def q_build(u):
        chosen = wide_lane == wide_row // own_heads * steps + u
        acc = None
        for h in range(0, own_heads, 2):
            one_hot = jnp.concatenate([jnp.where(chosen & (own_head == g), 1.0, 0.0) for g in (h, h + 1)], axis=1)
            pair = jnp.concatenate([q_own[h], q_own[h + 1]], axis=1)
            term = lax.dot_general(one_hot.astype(jnp.bfloat16), pair, (((1,), (1,)), ((), ())), preferred_element_type=jnp.float32)
            acc = term if acc is None else acc + term
        q_all[u, 0:group, me] = acc[:, :latent].astype(jnp.bfloat16).reshape(group, own_heads, latent)
        ropes = [acc[k * own_heads:(k + 1) * own_heads, latent:] for k in range(group)]
        q_all[u, group, me] = jnp.concatenate(ropes, axis=1).astype(jnp.bfloat16)

    def ag_own(u):
        q_build(u)
        ag_send_own(u)

    def ag_send_own(u):
        for kind in range(3):
            ag(u, kind).start()

    def ag_forward(u):
        ag(u, 0).wait_recv()
        ag(u, 3).start()
        ag(u, 4).start()
        ag(u, 1).wait_recv()
        ag(u, 5).start()

    def ag_relay(u):
        ag(u, 3).wait_recv()
        ag(u, 6).start()

    def ag_ready(u):
        pltpu.make_async_copy(q_all.at[u, :, 0:4], q_all.at[u, :, 0:4], ag_part.at[u]).wait()

    def d_copy(it, t):
        ring = it % RING
        return remote(o_tx.at[ring, D0 + t], rx_d.at[it, core], d_send.at[ring], d_recv.at[it % RX_RING], (x0, y1)[t])

    def pm_copy(it):
        ring, i = it % RING, it - LEAD
        return remote(o_tx.at[ring, PM], rx_d.at[i, 2], f_send.at[ring], d_recv.at[i % RX_RING], partner)

    def f_copy(it, t):
        ring, i = it % RING, it - LEAD
        return remote(o_tx.at[ring, (F0, F1, PF)[t]], rx_f.at[i, core if t < 2 else 2], f_send.at[ring], f_recv.at[it % RX_RING],
                      (x0, y1, partner)[t])

    def la_copy(it):
        ring, i = it % RING, it - LEAD
        return remote(lse_a.at[ring], rx_la.at[i], la_send.at[ring], la_recv.at[it % RX_RING], partner)

    def lb_copy(it, t):
        ring = it % RING
        return remote(lse_b.at[ring, t], rx_lb.at[it, core if t < 2 else 2], lb_send.at[ring], lb_recv.at[it % RX_RING], (x0, y1, partner)[t])

    def m_copy(it):
        ring, i = it % RING, it - LEAD
        return remote(m_tx.at[ring], rx_m.at[i], m_send.at[ring], m_recv.at[it % RX_RING], n1)

    def ml_copy(it):
        ring, i = it % RING, it - LEAD
        return remote(m_lse.at[ring], rx_ml.at[i], ml_send.at[ring], ml_recv.at[it % RX_RING], n1)

    def wait_bytes(ref, sem):
        pltpu.make_async_copy(ref, ref, sem).wait()

    def sent(it):
        ring = it % RING

        @pl.when(it < steps)
        def _():
            wait_bytes(o_tx.at[ring, 0:2], d_send.at[ring])

        @pl.when((it >= LEAD) & (it < steps + LEAD))
        def _():
            wait_bytes(o_tx.at[ring, 0:4], f_send.at[ring])
            wait_bytes(lse_a.at[ring], la_send.at[ring])
            wait_bytes(m_tx.at[ring], m_send.at[ring])
            wait_bytes(m_lse.at[ring], ml_send.at[ring])

        wait_bytes(lse_b.at[ring], lb_send.at[ring])

    lane = lax.broadcasted_iota(jnp.int32, (heads, 128), 1)
    col = lax.broadcasted_iota(jnp.int32, (1, page_len), 1)

    def attend(it, p, lse_row):
        slot = p % CACHE_SLOTS
        u, k = row(it, p), owners[p]
        c_load(it, p).wait()
        q = q_all[u, k].reshape(heads, latent)
        pair = q_all[u, group, :, :, pl.ds(pl.multiple_of(k // 2 * 128, 128), 128)].reshape(heads, 128)
        rope = jnp.where(k % 2 == 0, pair[:, :ROPE_DIM], pair[:, ROPE_DIM:])
        length = len_ref[k * steps + u]
        scores = []
        for j in range(pages):
            s = jnp.dot(q, cbuf[slot, j, :latent], preferred_element_type=jnp.float32)
            s = (s + jnp.dot(rope, cbuf[slot, j, latent:], preferred_element_type=jnp.float32)) * scale
            first = (j * group + me) * page_len
            scores.append(jnp.where(col + first < length, s, NEG))
        row_max = functools.reduce(jnp.maximum, [jnp.max(s, axis=1, keepdims=True) for s in scores])
        total = jnp.zeros((heads, 1), jnp.float32)
        acc = jnp.zeros((heads, latent), jnp.float32)
        for j in range(pages):
            w = jnp.exp(scores[j] - row_max)
            total = total + jnp.sum(w, axis=1, keepdims=True)
            acc = acc + lax.dot_general(w.astype(jnp.bfloat16), cbuf[slot, j, :latent], (((1,), (1,)), ((), ())),
                                        preferred_element_type=jnp.float32)
        o_tx[it % RING, p] = (acc / total).astype(jnp.bfloat16)
        lse_acc[...] = jnp.where(lane == lse_row, row_max + jnp.log(total), lse_acc[...])

    def weighted(rows, blocks):
        top = functools.reduce(jnp.maximum, rows)
        total = functools.reduce(jnp.add, [jnp.exp(v - top) for v in rows])
        lse = top + jnp.log(total)
        for n, v in enumerate(rows):
            w_rows[n:n + 1, :] = jnp.exp(v - lse)
        cols = w_rows[...].T
        acc = cols[:, 0:1] * blocks[0].astype(jnp.float32)
        for n in range(1, len(blocks)):
            acc = acc + cols[:, n:n + 1] * blocks[n].astype(jnp.float32)
        return lse, acc

    def merge(it):
        ring, i = it % RING, it - LEAD
        wait_bytes(rx_d.at[i], d_recv.at[i % RX_RING])
        wait_bytes(rx_lb.at[i], lb_recv.at[i % RX_RING])
        wait_bytes(rx_la.at[i], la_recv.at[it % RX_RING])
        rows = [lse_a[ring][0:1], rx_lb[i, 0][0:1], rx_lb[i, 1][0:1], rx_la[i][1:2]]
        lse, acc = weighted(rows, [o_tx[ring, OM], rx_d[i, 0], rx_d[i, 1], rx_d[i, 2]])
        m_tx[ring] = acc
        m_lse[ring] = lse

    def final(it):
        ring, i = it % RING, it - LEAD
        wait_bytes(rx_f.at[i], f_recv.at[it % RX_RING])

        @pl.when(it >= steps)
        def _():
            wait_bytes(rx_lb.at[it], lb_recv.at[it % RX_RING])

        wait_bytes(rx_m.at[i], m_recv.at[it % RX_RING])
        wait_bytes(rx_ml.at[i], ml_recv.at[it % RX_RING])
        rows = [lse_b[ring, 2][1:2], rx_lb[it, 0][1:2], rx_lb[it, 1][1:2], rx_lb[it, 2][0:1], rx_ml[i]]
        _, acc = weighted(rows, [o_tx[ring, OF], rx_f[i, 0], rx_f[i, 1], rx_f[i, 2], rx_m[i]])
        o_stage[i % 2] = acc.astype(jnp.bfloat16)

    q_load().start()
    len_load().start()
    for p in range(CACHE_SLOTS - 1):
        if p in (D0, D1):
            c_load(0, p).start()

    w_rows[...] = jnp.zeros_like(w_rows)
    lse_acc[...] = jnp.zeros_like(lse_acc)
    q_load().wait()
    q_build(0)
    pl.semaphore_wait(barrier, len(peers))

    ag_send_own(0)
    ag_own(1)
    ag_forward(0)
    ag_own(2)
    ag_own(3)
    ag_forward(1)
    ag_relay(0)
    len_load().wait()

    def gather(it, phase):
        if phase == 0:
            @pl.when(it < steps // 2 - 2)
            def _():
                ag_own(2 * it + 4)
                ag_own(2 * it + 5)
        elif phase == 1:
            @pl.when(it < steps // 2 - 1)
            def _():
                ag_forward(2 * it + 2)
                ag_forward(2 * it + 3)
        else:
            @pl.when((it >= 1) & (it < steps // 2))
            def _():
                ag_relay(2 * it)

            @pl.when(it < steps // 2)
            def _():
                ag_relay(2 * it + 1)

    @pl.loop(0, steps + LEAD + FINAL_LAG)
    def _(it):
        @pl.when(it >= RING)
        def _():
            sent(it - RING)

        @pl.when(it < steps)
        def _():
            ag_ready(it)

        gather(it, 0)
        for p in range(group):
            ahead = p + CACHE_SLOTS - 1
            nxt = it + ahead // group

            @pl.when(valid(nxt, ahead % group))
            def _():
                c_load(nxt, ahead % group).start()

            @pl.when(valid(it, p))
            def _():
                attend(it, p, (6, 7, 0, 2, 1, 3, 4, 5)[p])
                if p == PM:
                    lse_a[it % RING] = lse_acc[...].T[6:8]
                    pm_copy(it).start()
                    la_copy(it).start()
                elif p in (D0, D1):
                    d_copy(it, p - D0).start()
                elif p in (F0, F1):
                    f_copy(it, p - F0).start()
                elif p == PF:
                    f_copy(it, 2).start()
                if p == F1:
                    merge(it)
                    m_copy(it).start()
                    ml_copy(it).start()

            if p == D1:
                gather(it, 1)
            if p == F1:
                gather(it, 2)

        @pl.when(it < steps + LEAD)
        def _():
            rows = lse_acc[...].T
            for t in range(3):
                lse_b[it % RING, t] = rows[2 * t:2 * t + 2]
            for t in range(3):
                lb_copy(it, t).start()

        @pl.when(it >= LEAD + FINAL_LAG)
        def _():
            k = it - FINAL_LAG

            @pl.when(k >= LEAD + 2)
            def _():
                out_copy(k - LEAD - 2).wait()

            final(k)
            out_copy(k - LEAD).start()

    @pl.loop(steps + LEAD + FINAL_LAG - RING, steps + LEAD)
    def _(it):
        sent(it)

    for kind in range(7):
        wait_bytes(q_all.at[:, :, kind], ag_send.at[kind])

    for i in (steps - 2, steps - 1):
        out_copy(i).wait()


def _hand_over(src, dst, buf, in_sem, out_sem):
    rows = src.shape[0] // 4
    parts = [pl.ds(k * rows, rows) for k in range(4)]
    loads = [pltpu.make_async_copy(src.at[p], buf.at[p], in_sem.at[k]) for k, p in enumerate(parts)]
    stores = [pltpu.make_async_copy(buf.at[p], dst.at[p], out_sem.at[k]) for k, p in enumerate(parts)]
    for load in loads:
        load.start()
    for load, store in zip(loads, stores):
        load.wait()
        store.start()
    for store in stores:
        store.wait()


def solution(mesh):
    group = mesh.shape['dcp']

    def local_step(q_blk, cache_blk, len_blk):
        batch, own_heads, width = q_blk.shape
        pages, page_len = cache_blk.shape[1], cache_blk.shape[3]
        steps = batch // group
        heads = own_heads * group
        latent = width - ROPE_DIM
        bf16, f32 = jnp.bfloat16, jnp.float32
        dma = pltpu.SemaphoreType.DMA
        merged = pl.pallas_call(
            functools.partial(_kernel, (steps, group, heads, latent, pages, page_len)),
            out_shape=jax.ShapeDtypeStruct((steps, heads, latent), bf16),
            in_specs=[pl.BlockSpec(memory_space=pl.ANY)] * 3,
            out_specs=pl.BlockSpec(memory_space=pl.ANY),
            scratch_shapes=[
                pltpu.SMEM((batch,), jnp.int32),
                pltpu.VMEM((own_heads, width, batch), bf16),
                pltpu.VMEM((steps, group + 1, group, own_heads, latent), bf16),
                pltpu.VMEM((CACHE_SLOTS, pages, width, page_len), bf16),
                pltpu.VMEM((RING, group, heads, latent), bf16),
                pltpu.VMEM((heads, 128), f32),
                pltpu.VMEM((RING, 2, heads), f32),
                pltpu.VMEM((RING, 3, 2, heads), f32),
                pltpu.VMEM((steps, 3, heads, latent), bf16),
                pltpu.VMEM((steps, 3, heads, latent), bf16),
                pltpu.VMEM((steps, 2, heads), f32),
                pltpu.VMEM((steps + LEAD, 3, 2, heads), f32),
                pltpu.VMEM((RING, heads, latent), f32),
                pltpu.VMEM((RING, 1, heads), f32),
                pltpu.VMEM((steps, heads, latent), f32),
                pltpu.VMEM((steps, 1, heads), f32),
                pltpu.VMEM((128, heads), f32),
                pltpu.VMEM((2, heads, latent), bf16),
                dma, dma, dma((CACHE_SLOTS,)), dma((2,)),
                dma((7,)), dma((AG_RING, 3)), dma((steps,)),
                *[dma((RING,))] * 6, *[dma((RX_RING,))] * 6,
            ],
            compiler_params=pltpu.CompilerParams(collective_id=0, has_side_effects=True, vmem_limit_bytes=66_000_000),
        )(len_blk, jnp.transpose(q_blk, (1, 2, 0)), jnp.swapaxes(cache_blk, 3, 4))
        return pl.pallas_call(
            _hand_over, out_shape=jax.ShapeDtypeStruct((steps, heads, latent), bf16),
            in_specs=[pl.BlockSpec(memory_space=pl.ANY)], out_specs=pl.BlockSpec(memory_space=pl.ANY),
            scratch_shapes=[pltpu.VMEM((steps, heads, latent), bf16), dma((4,)), dma((4,))])(merged)

    return jax.shard_map(local_step, mesh=mesh, in_specs=(P('dp', 'dcp', None), P('dp', None, 'dcp', None, None), P('dp')),
                         out_specs=P(('dp', 'dcp'), None, None), check_vma=False)
```

```python
import functools

import jax
import jax.numpy as jnp
from jax import lax
from jax.experimental import pallas as pl
from jax.experimental.pallas import tpu as pltpu
from jax.sharding import PartitionSpec as P

ROPE_DIM = 64
QK_DIM = 192
MESH = pl.DeviceIdType.MESH
NEG = -1e30

CACHE_SLOTS = 4
RING = 4
AG_RING = 8
RX_RING = 8
VMEM_BYTES = 54_000_000
Q_PART = 4
LEAD = 2
FINAL_LAG = 2


def _kernel(dims, len_hbm, q_hbm, cache_ref, out_ref, len_ref, q_own, q_all, cbuf, o_tx, lse_acc, lse_a, lse_b, rx_d, rx_f, rx_la, rx_lb,
            m_tx, m_lse, rx_m, rx_ml, w_rows, len_sem, q_sem, c_sem, ag_send, ag_recv, ag_part,
            d_send, f_send, la_send, lb_send, m_send, ml_send, d_recv, f_recv, la_recv, lb_recv, m_recv, ml_recv):
    steps, group, heads, latent, pages, page_len = dims
    scale = QK_DIM ** -0.5
    me = lax.axis_index('dcp')
    core = me % 2
    x = (me // 2) % 2
    y = me // 4

    def dev(dx, dy, c):
        return ((y + dy) % 2 * 2 + (x + dx) % 2) * 2 + c

    n1x, n1y = core, 1 - core
    n2x, n2y = 1 - core, core
    n1 = dev(n1x, n1y, core)
    n2 = dev(n2x, n2y, core)
    partner = dev(0, 0, 1 - core)
    diag = dev(1, 1, core)
    x0, y1 = dev(1, 0, 0), dev(0, 1, 1)

    OM, PM, D0, D1, F0, F1, PF, OF = range(8)
    owners = (
        dev(n1x, n1y, core),
        dev(n2x, n2y, 1 - core),
        dev(1, 1, 0), dev(1, 1, 1),
        x0, y1,
        partner, me,
    )

    def remote(src, dst, send, recv, device):
        return pltpu.make_async_remote_copy(src_ref=src, dst_ref=dst, send_sem=send, recv_sem=recv,
                                            device_id={'dcp': device}, device_id_type=MESH)

    barrier = pltpu.get_barrier_semaphore()
    peers = (n1, n2, partner)
    for peer in peers:
        pl.semaphore_signal(barrier, inc=1, device_id={'dcp': peer}, device_id_type=MESH)

    def len_load():
        return pltpu.make_async_copy(len_hbm, len_ref, len_sem)

    def q_load(part):
        some = pl.ds(part * Q_PART, Q_PART)
        return pltpu.make_async_copy(q_hbm.at[some], q_own.at[some], q_sem.at[part])

    def row(it, p):
        return it if p in (D0, D1) else it - LEAD

    def valid(it, p):
        return it < steps if p in (D0, D1) else (it >= LEAD) & (it < steps + LEAD)

    def c_load(it, p):
        slot = p % CACHE_SLOTS
        return pltpu.make_async_copy(cache_ref.at[owners[p] * steps + row(it, p), :, 0], cbuf.at[slot], c_sem.at[slot])

    def ag(u, kind):
        block = (me, me, me, n2, n2, n1, diag)[kind]
        target = (n2, n1, partner, n1, partner, partner, partner)[kind]
        recv = ag_part.at[u] if kind in (2, 4, 5, 6) else ag_recv.at[u % AG_RING, (0, 1, None, 2)[kind]]
        return remote(q_all.at[u, :, block], q_all.at[u, :, block], ag_send.at[kind], recv, target)

    wide_row = lax.broadcasted_iota(jnp.int32, (heads, steps * group), 0)
    wide_lane = lax.broadcasted_iota(jnp.int32, (heads, steps * group), 1)
    own_heads = heads // group
    own_head = wide_row % own_heads

    def q_build(u, loading=False):
        chosen = wide_lane == wide_row // own_heads * steps + u
        acc = None
        for h in range(0, own_heads, 2):
            if loading and h % Q_PART == 0:
                q_load(h // Q_PART).wait()
            one_hot = jnp.concatenate([jnp.where(chosen & (own_head == g), 1.0, 0.0) for g in (h, h + 1)], axis=1)
            pair = jnp.concatenate([q_own[h], q_own[h + 1]], axis=1)
            term = lax.dot_general(one_hot.astype(jnp.bfloat16), pair, (((1,), (1,)), ((), ())), preferred_element_type=jnp.float32)
            acc = term if acc is None else acc + term
        q_all[u, 0:group, me] = acc[:, :latent].astype(jnp.bfloat16).reshape(group, own_heads, latent)
        ropes = [acc[k * own_heads:(k + 1) * own_heads, latent:] for k in range(group)]
        q_all[u, group, me] = jnp.concatenate(ropes, axis=1).astype(jnp.bfloat16)

    def ag_own(u):
        q_build(u)
        ag_send_own(u)

    def ag_send_own(u):
        for kind in range(3):
            ag(u, kind).start()

    def ag_forward(u):
        ag(u, 0).wait_recv()
        ag(u, 3).start()
        ag(u, 4).start()
        ag(u, 1).wait_recv()
        ag(u, 5).start()

    def ag_relay(u):
        ag(u, 3).wait_recv()
        ag(u, 6).start()

    def ag_ready(u):
        pltpu.make_async_copy(q_all.at[u, :, 0:4], q_all.at[u, :, 0:4], ag_part.at[u]).wait()

    def d_copy(it, t):
        ring = it % RING
        return remote(o_tx.at[ring, D0 + t], rx_d.at[it, core], d_send.at[ring], d_recv.at[it % RX_RING], (x0, y1)[t])

    def pm_copy(it):
        ring, i = it % RING, it - LEAD
        return remote(o_tx.at[ring, PM], rx_d.at[i, 2], f_send.at[ring], d_recv.at[i % RX_RING], partner)

    def f_copy(it, t):
        ring, i = it % RING, it - LEAD
        return remote(o_tx.at[ring, (F0, F1, PF)[t]], rx_f.at[i, core if t < 2 else 2], f_send.at[ring], f_recv.at[it % RX_RING],
                      (x0, y1, partner)[t])

    def la_copy(it):
        ring, i = it % RING, it - LEAD
        return remote(lse_a.at[ring], rx_la.at[i], la_send.at[ring], la_recv.at[it % RX_RING], partner)

    def lb_copy(it, t):
        ring = it % RING
        return remote(lse_b.at[ring, t], rx_lb.at[it, core if t < 2 else 2], lb_send.at[ring], lb_recv.at[it % RX_RING], (x0, y1, partner)[t])

    def m_copy(it):
        ring, i = it % RING, it - LEAD
        return remote(m_tx.at[ring], rx_m.at[i], m_send.at[ring], m_recv.at[it % RX_RING], n1)

    def ml_copy(it):
        ring, i = it % RING, it - LEAD
        return remote(m_lse.at[ring], rx_ml.at[i], ml_send.at[ring], ml_recv.at[it % RX_RING], n1)

    def wait_bytes(ref, sem):
        pltpu.make_async_copy(ref, ref, sem).wait()

    def sent(it):
        ring = it % RING

        @pl.when(it < steps)
        def _():
            wait_bytes(o_tx.at[ring, 0:2], d_send.at[ring])

        @pl.when((it >= LEAD) & (it < steps + LEAD))
        def _():
            wait_bytes(o_tx.at[ring, 0:4], f_send.at[ring])
            wait_bytes(lse_a.at[ring], la_send.at[ring])
            wait_bytes(m_tx.at[ring], m_send.at[ring])
            wait_bytes(m_lse.at[ring], ml_send.at[ring])

        wait_bytes(lse_b.at[ring], lb_send.at[ring])

    lane = lax.broadcasted_iota(jnp.int32, (heads, 128), 1)
    col = lax.broadcasted_iota(jnp.int32, (1, page_len), 1)

    def attend(it, p, lse_row):
        slot = p % CACHE_SLOTS
        u, k = row(it, p), owners[p]
        c_load(it, p).wait()
        q = q_all[u, k].reshape(heads, latent)
        pair = q_all[u, group, :, :, pl.ds(pl.multiple_of(k // 2 * 128, 128), 128)].reshape(heads, 128)
        rope = jnp.where(k % 2 == 0, pair[:, :ROPE_DIM], pair[:, ROPE_DIM:])
        length = len_ref[k * steps + u]
        scores = []
        for j in range(pages):
            s = jnp.dot(q, cbuf[slot, j, :latent], preferred_element_type=jnp.float32)
            s = (s + jnp.dot(rope, cbuf[slot, j, latent:], preferred_element_type=jnp.float32)) * scale
            first = (j * group + me) * page_len
            scores.append(jnp.where(col + first < length, s, NEG))
        row_max = functools.reduce(jnp.maximum, [jnp.max(s, axis=1, keepdims=True) for s in scores])
        total = jnp.zeros((heads, 1), jnp.float32)
        acc = jnp.zeros((heads, latent), jnp.float32)
        for j in range(pages):
            w = jnp.exp(scores[j] - row_max)
            total = total + jnp.sum(w, axis=1, keepdims=True)
            acc = acc + lax.dot_general(w.astype(jnp.bfloat16), cbuf[slot, j, :latent], (((1,), (1,)), ((), ())),
                                        preferred_element_type=jnp.float32)
        o_tx[it % RING, p] = (acc / total).astype(jnp.bfloat16)
        lse_acc[...] = jnp.where(lane == lse_row, row_max + jnp.log(total), lse_acc[...])

    def weighted(rows, blocks):
        top = functools.reduce(jnp.maximum, rows)
        total = functools.reduce(jnp.add, [jnp.exp(v - top) for v in rows])
        lse = top + jnp.log(total)
        for n, v in enumerate(rows):
            w_rows[n:n + 1, :] = jnp.exp(v - lse)
        cols = w_rows[...].T
        acc = cols[:, 0:1] * blocks[0].astype(jnp.float32)
        for n in range(1, len(blocks)):
            acc = acc + cols[:, n:n + 1] * blocks[n].astype(jnp.float32)
        return lse, acc

    def merge(it):
        ring, i = it % RING, it - LEAD
        wait_bytes(rx_d.at[i], d_recv.at[i % RX_RING])
        wait_bytes(rx_lb.at[i], lb_recv.at[i % RX_RING])
        wait_bytes(rx_la.at[i], la_recv.at[it % RX_RING])
        rows = [lse_a[ring][0:1], rx_lb[i, 0][0:1], rx_lb[i, 1][0:1], rx_la[i][1:2]]
        lse, acc = weighted(rows, [o_tx[ring, OM], rx_d[i, 0], rx_d[i, 1], rx_d[i, 2]])
        m_tx[ring] = acc
        m_lse[ring] = lse

    def final(it):
        ring, i = it % RING, it - LEAD
        wait_bytes(rx_f.at[i], f_recv.at[it % RX_RING])

        @pl.when(it >= steps)
        def _():
            wait_bytes(rx_lb.at[it], lb_recv.at[it % RX_RING])

        wait_bytes(rx_m.at[i], m_recv.at[it % RX_RING])
        wait_bytes(rx_ml.at[i], ml_recv.at[it % RX_RING])
        rows = [lse_b[ring, 2][1:2], rx_lb[it, 0][1:2], rx_lb[it, 1][1:2], rx_lb[it, 2][0:1], rx_ml[i]]
        _, acc = weighted(rows, [o_tx[ring, OF], rx_f[i, 0], rx_f[i, 1], rx_f[i, 2], rx_m[i]])
        out_ref[i] = acc.astype(jnp.bfloat16)

    for part in range(own_heads // Q_PART):
        q_load(part).start()

    w_rows[...] = jnp.zeros_like(w_rows)
    lse_acc[...] = jnp.zeros_like(lse_acc)
    q_build(0, loading=True)
    pl.semaphore_wait(barrier, len(peers))

    ag_send_own(0)
    len_load().start()
    for p in range(CACHE_SLOTS - 1):
        if p in (D0, D1):
            c_load(0, p).start()
    ag_own(1)
    ag_forward(0)
    ag_own(2)
    ag_own(3)
    ag_forward(1)
    ag_relay(0)
    len_load().wait()

    def gather(it, phase):
        if phase == 0:
            @pl.when(it < steps // 2 - 2)
            def _():
                ag_own(2 * it + 4)
                ag_own(2 * it + 5)
        elif phase == 1:
            @pl.when(it < steps // 2 - 1)
            def _():
                ag_forward(2 * it + 2)
                ag_forward(2 * it + 3)
        else:
            @pl.when((it >= 1) & (it < steps // 2))
            def _():
                ag_relay(2 * it)

            @pl.when(it < steps // 2)
            def _():
                ag_relay(2 * it + 1)

    @pl.loop(0, steps + LEAD + FINAL_LAG)
    def _(it):
        @pl.when(it >= RING)
        def _():
            sent(it - RING)

        @pl.when(it < steps)
        def _():
            ag_ready(it)

        gather(it, 0)
        for p in range(group):
            ahead = p + CACHE_SLOTS - 1
            nxt = it + ahead // group

            @pl.when(valid(nxt, ahead % group))
            def _():
                c_load(nxt, ahead % group).start()

            @pl.when(valid(it, p))
            def _():
                attend(it, p, (6, 7, 0, 2, 1, 3, 4, 5)[p])
                if p == PM:
                    lse_a[it % RING] = lse_acc[...].T[6:8]
                    pm_copy(it).start()
                    la_copy(it).start()
                elif p in (D0, D1):
                    d_copy(it, p - D0).start()
                elif p in (F0, F1):
                    f_copy(it, p - F0).start()
                elif p == PF:
                    f_copy(it, 2).start()
                if p == F1:
                    merge(it)
                    m_copy(it).start()
                    ml_copy(it).start()

            if p == D1:
                gather(it, 1)
            if p == F1:
                gather(it, 2)

        @pl.when(it < steps + LEAD)
        def _():
            rows = lse_acc[...].T
            for t in range(3):
                lse_b[it % RING, t] = rows[2 * t:2 * t + 2]
            for t in range(3):
                lb_copy(it, t).start()

        @pl.when(it >= LEAD + FINAL_LAG)
        def _():
            k = it - FINAL_LAG

            final(k)

    @pl.loop(steps + LEAD + FINAL_LAG - RING, steps + LEAD)
    def _(it):
        sent(it)

    for kind in range(7):
        wait_bytes(q_all.at[:, :, kind], ag_send.at[kind])


def solution(mesh):
    group = mesh.shape['dcp']

    def local_step(q_blk, cache_blk, len_blk):
        batch, own_heads, width = q_blk.shape
        pages, page_len = cache_blk.shape[1], cache_blk.shape[3]
        steps = batch // group
        heads = own_heads * group
        latent = width - ROPE_DIM
        bf16, f32 = jnp.bfloat16, jnp.float32
        dma = pltpu.SemaphoreType.DMA
        return pl.pallas_call(
            functools.partial(_kernel, (steps, group, heads, latent, pages, page_len)),
            out_shape=jax.ShapeDtypeStruct((steps, heads, latent), bf16),
            in_specs=[pl.BlockSpec(memory_space=pltpu.HBM)] * 3,
            out_specs=pl.BlockSpec(memory_space=pltpu.VMEM),
            scratch_shapes=[
                pltpu.SMEM((batch,), jnp.int32),
                pltpu.VMEM((own_heads, width, batch), bf16),
                pltpu.VMEM((steps, group + 1, group, own_heads, latent), bf16),
                pltpu.VMEM((CACHE_SLOTS, pages, width, page_len), bf16),
                pltpu.VMEM((RING, group, heads, latent), bf16),
                pltpu.VMEM((heads, 128), f32),
                pltpu.VMEM((RING, 2, heads), f32),
                pltpu.VMEM((RING, 3, 2, heads), f32),
                pltpu.VMEM((steps, 3, heads, latent), bf16),
                pltpu.VMEM((steps, 3, heads, latent), bf16),
                pltpu.VMEM((steps, 2, heads), f32),
                pltpu.VMEM((steps + LEAD, 3, 2, heads), f32),
                pltpu.VMEM((RING, heads, latent), f32),
                pltpu.VMEM((RING, 1, heads), f32),
                pltpu.VMEM((steps, heads, latent), f32),
                pltpu.VMEM((steps, 1, heads), f32),
                pltpu.VMEM((128, heads), f32),
                dma, dma((own_heads // Q_PART,)), dma((CACHE_SLOTS,)),
                dma((7,)), dma((AG_RING, 3)), dma((steps,)),
                *[dma((RING,))] * 6, *[dma((RX_RING,))] * 6,
            ],
            compiler_params=pltpu.CompilerParams(collective_id=0, has_side_effects=True, vmem_limit_bytes=VMEM_BYTES),
        )(len_blk, jnp.transpose(q_blk, (1, 2, 0)), jnp.swapaxes(cache_blk, 3, 4))

    return jax.shard_map(local_step, mesh=mesh, in_specs=(P('dp', 'dcp', None), P('dp', None, 'dcp', None, None), P('dp')),
                         out_specs=P(('dp', 'dcp'), None, None), check_vma=False)
```

```python
import functools

import jax
import jax.numpy as jnp
from jax import lax
from jax.experimental import pallas as pl
from jax.experimental.pallas import tpu as pltpu
from jax.sharding import PartitionSpec as P

ROPE_DIM = 64
QK_DIM = 192
MESH = pl.DeviceIdType.MESH
NEG = -1e30

CACHE_SLOTS = 4
RING = 4
AG_RING = 8
RX_RING = 8
VMEM_BYTES = 54_000_000
Q_PART = 4
LEAD = 2
FINAL_LAG = 2


def _kernel(dims, len_hbm, q_hbm, cache_ref, out_ref, len_ref, q_own, q_all, cbuf, o_tx, lse_acc, lse_a, lse_b, rx_d, rx_f, rx_la, rx_lb,
            m_tx, m_lse, rx_m, rx_ml, w_rows, len_sem, q_sem, c_sem, ag_send, ag_recv, ag_part,
            d_send, f_send, la_send, lb_send, m_send, ml_send, d_recv, f_recv, la_recv, lb_recv, m_recv, ml_recv):
    steps, group, heads, latent, pages, page_len = dims
    scale = QK_DIM ** -0.5
    me = lax.axis_index('dcp')
    core = me % 2
    x = (me // 2) % 2
    y = me // 4

    def dev(dx, dy, c):
        return ((y + dy) % 2 * 2 + (x + dx) % 2) * 2 + c

    n1x, n1y = core, 1 - core
    n2x, n2y = 1 - core, core
    n1 = dev(n1x, n1y, core)
    n2 = dev(n2x, n2y, core)
    partner = dev(0, 0, 1 - core)
    diag = dev(1, 1, core)
    x0, y1 = dev(1, 0, 0), dev(0, 1, 1)

    OM, PM, D0, D1, F0, F1, PF, OF = range(8)
    owners = (
        dev(n1x, n1y, core),
        dev(n2x, n2y, 1 - core),
        dev(1, 1, 0), dev(1, 1, 1),
        x0, y1,
        partner, me,
    )

    def remote(src, dst, send, recv, device):
        return pltpu.make_async_remote_copy(src_ref=src, dst_ref=dst, send_sem=send, recv_sem=recv,
                                            device_id={'dcp': device}, device_id_type=MESH)

    barrier = pltpu.get_barrier_semaphore()
    peers = (n1, n2, partner)
    for peer in peers:
        pl.semaphore_signal(barrier, inc=1, device_id={'dcp': peer}, device_id_type=MESH)

    def len_load():
        return pltpu.make_async_copy(len_hbm, len_ref, len_sem)

    def q_load(part):
        some = pl.ds(part * Q_PART, Q_PART)
        return pltpu.make_async_copy(q_hbm.at[some], q_own.at[some], q_sem.at[part])

    def row(it, p):
        return it if p in (D0, D1) else it - LEAD

    def valid(it, p):
        return it < steps if p in (D0, D1) else (it >= LEAD) & (it < steps + LEAD)

    def c_load(it, p):
        slot = p % CACHE_SLOTS
        return pltpu.make_async_copy(cache_ref.at[owners[p] * steps + row(it, p), :, 0], cbuf.at[slot], c_sem.at[slot])

    def ag(u, kind):
        block = (me, me, me, n2, n2, n1, diag)[kind]
        target = (n2, n1, partner, n1, partner, partner, partner)[kind]
        recv = ag_part.at[u] if kind in (2, 4, 5, 6) else ag_recv.at[u % AG_RING, (0, 1, None, 2)[kind]]
        return remote(q_all.at[u, :, block], q_all.at[u, :, block], ag_send.at[kind], recv, target)

    wide_row = lax.broadcasted_iota(jnp.int32, (heads, steps * group), 0)
    wide_lane = lax.broadcasted_iota(jnp.int32, (heads, steps * group), 1)
    own_heads = heads // group
    own_head = wide_row % own_heads

    def q_build(u, loading=False):
        chosen = wide_lane == wide_row // own_heads * steps + u
        acc = None
        for h in range(0, own_heads, 2):
            if loading and h % Q_PART == 0:
                q_load(h // Q_PART).wait()
            one_hot = jnp.concatenate([jnp.where(chosen & (own_head == g), 1.0, 0.0) for g in (h, h + 1)], axis=1)
            pair = jnp.concatenate([q_own[h], q_own[h + 1]], axis=1)
            term = lax.dot_general(one_hot.astype(jnp.bfloat16), pair, (((1,), (1,)), ((), ())), preferred_element_type=jnp.float32)
            acc = term if acc is None else acc + term
        q_all[u, 0:group, me] = acc[:, :latent].astype(jnp.bfloat16).reshape(group, own_heads, latent)
        ropes = [acc[k * own_heads:(k + 1) * own_heads, latent:] for k in range(group)]
        q_all[u, group, me] = jnp.concatenate(ropes, axis=1).astype(jnp.bfloat16)

    def ag_own(u):
        q_build(u)
        ag_send_own(u)

    def ag_send_own(u):
        for kind in range(3):
            ag(u, kind).start()

    def ag_forward(u):
        ag(u, 0).wait_recv()
        ag(u, 3).start()
        ag(u, 4).start()
        ag(u, 1).wait_recv()
        ag(u, 5).start()

    def ag_relay(u):
        ag(u, 3).wait_recv()
        ag(u, 6).start()

    def ag_ready(u):
        pltpu.make_async_copy(q_all.at[u, :, 0:4], q_all.at[u, :, 0:4], ag_part.at[u]).wait()

    def d_copy(it, t):
        ring = it % RING
        return remote(o_tx.at[ring, D0 + t], rx_d.at[it, core], d_send.at[ring], d_recv.at[it % RX_RING], (x0, y1)[t])

    def pm_copy(it):
        ring, i = it % RING, it - LEAD
        return remote(o_tx.at[ring, PM], rx_d.at[i, 2], f_send.at[ring], d_recv.at[i % RX_RING], partner)

    def f_copy(it, t):
        ring, i = it % RING, it - LEAD
        return remote(o_tx.at[ring, (F0, F1, PF)[t]], rx_f.at[i, core if t < 2 else 2], f_send.at[ring], f_recv.at[it % RX_RING],
                      (x0, y1, partner)[t])

    def la_copy(it):
        ring, i = it % RING, it - LEAD
        return remote(lse_a.at[ring], rx_la.at[i], la_send.at[ring], la_recv.at[it % RX_RING], partner)

    def lb_copy(it, t):
        ring = it % RING
        return remote(lse_b.at[ring, t], rx_lb.at[it, core if t < 2 else 2], lb_send.at[ring], lb_recv.at[it % RX_RING], (x0, y1, partner)[t])

    def m_copy(it):
        ring, i = it % RING, it - LEAD
        return remote(m_tx.at[ring], rx_m.at[i], m_send.at[ring], m_recv.at[it % RX_RING], n1)

    def ml_copy(it):
        ring, i = it % RING, it - LEAD
        return remote(m_lse.at[ring], rx_ml.at[i], ml_send.at[ring], ml_recv.at[it % RX_RING], n1)

    def wait_bytes(ref, sem):
        pltpu.make_async_copy(ref, ref, sem).wait()

    def sent(it):
        ring = it % RING

        @pl.when(it < steps)
        def _():
            wait_bytes(o_tx.at[ring, 0:2], d_send.at[ring])

        @pl.when((it >= LEAD) & (it < steps + LEAD))
        def _():
            wait_bytes(o_tx.at[ring, 0:4], f_send.at[ring])
            wait_bytes(lse_a.at[ring], la_send.at[ring])
            wait_bytes(m_tx.at[ring], m_send.at[ring])
            wait_bytes(m_lse.at[ring], ml_send.at[ring])

        wait_bytes(lse_b.at[ring], lb_send.at[ring])

    lane = lax.broadcasted_iota(jnp.int32, (heads, 128), 1)
    col = lax.broadcasted_iota(jnp.int32, (1, page_len), 1)

    def attend(it, p, lse_row):
        slot = p % CACHE_SLOTS
        u, k = row(it, p), owners[p]
        c_load(it, p).wait()
        q = q_all[u, k].reshape(heads, latent)
        pair = q_all[u, group, :, :, pl.ds(pl.multiple_of(k // 2 * 128, 128), 128)].reshape(heads, 128)
        rope = jnp.where(k % 2 == 0, pair[:, :ROPE_DIM], pair[:, ROPE_DIM:])
        length = len_ref[k * steps + u]
        scores = []
        for j in range(pages):
            s = jnp.dot(q, cbuf[slot, j, :latent], preferred_element_type=jnp.float32)
            s = (s + jnp.dot(rope, cbuf[slot, j, latent:], preferred_element_type=jnp.float32)) * scale
            first = (j * group + me) * page_len
            scores.append(jnp.where(col + first < length, s, NEG))
        row_max = functools.reduce(jnp.maximum, [jnp.max(s, axis=1, keepdims=True) for s in scores])
        total = jnp.zeros((heads, 1), jnp.float32)
        acc = jnp.zeros((heads, latent), jnp.float32)
        for j in range(pages):
            w = jnp.exp(scores[j] - row_max)
            total = total + jnp.sum(w, axis=1, keepdims=True)
            acc = acc + lax.dot_general(w.astype(jnp.bfloat16), cbuf[slot, j, :latent], (((1,), (1,)), ((), ())),
                                        preferred_element_type=jnp.float32)
        o_tx[it % RING, p] = (acc / total).astype(jnp.bfloat16)
        lse_acc[...] = jnp.where(lane == lse_row, row_max + jnp.log(total), lse_acc[...])

    def weighted(rows, blocks):
        top = functools.reduce(jnp.maximum, rows)
        total = functools.reduce(jnp.add, [jnp.exp(v - top) for v in rows])
        lse = top + jnp.log(total)
        for n, v in enumerate(rows):
            w_rows[n:n + 1, :] = jnp.exp(v - lse)
        cols = w_rows[...].T
        acc = cols[:, 0:1] * blocks[0].astype(jnp.float32)
        for n in range(1, len(blocks)):
            acc = acc + cols[:, n:n + 1] * blocks[n].astype(jnp.float32)
        return lse, acc

    def merge(it):
        ring, i = it % RING, it - LEAD
        wait_bytes(rx_d.at[i], d_recv.at[i % RX_RING])
        wait_bytes(rx_lb.at[i], lb_recv.at[i % RX_RING])
        wait_bytes(rx_la.at[i], la_recv.at[it % RX_RING])
        rows = [lse_a[ring][0:1], rx_lb[i, 0][0:1], rx_lb[i, 1][0:1], rx_la[i][1:2]]
        lse, acc = weighted(rows, [o_tx[ring, OM], rx_d[i, 0], rx_d[i, 1], rx_d[i, 2]])
        m_tx[ring] = acc
        m_lse[ring] = lse

    def final(it):
        ring, i = it % RING, it - LEAD
        wait_bytes(rx_f.at[i], f_recv.at[it % RX_RING])

        @pl.when(it >= steps)
        def _():
            wait_bytes(rx_lb.at[it], lb_recv.at[it % RX_RING])

        wait_bytes(rx_m.at[i], m_recv.at[it % RX_RING])
        wait_bytes(rx_ml.at[i], ml_recv.at[it % RX_RING])
        rows = [lse_b[ring, 2][1:2], rx_lb[it, 0][1:2], rx_lb[it, 1][1:2], rx_lb[it, 2][0:1], rx_ml[i]]
        _, acc = weighted(rows, [o_tx[ring, OF], rx_f[i, 0], rx_f[i, 1], rx_f[i, 2], rx_m[i]])
        out_ref[i] = acc.astype(jnp.bfloat16)

    for part in range(own_heads // Q_PART):
        q_load(part).start()

    w_rows[...] = jnp.zeros_like(w_rows)
    lse_acc[...] = jnp.zeros_like(lse_acc)
    q_build(0, loading=True)
    pl.semaphore_wait(barrier, len(peers))

    ag_send_own(0)
    len_load().start()
    for p in range(CACHE_SLOTS - 1):
        if p in (D0, D1):
            c_load(0, p).start()
    ag_own(1)
    ag_forward(0)
    ag_own(2)
    ag_own(3)
    ag_forward(1)
    ag_relay(0)
    len_load().wait()

    def gather(it, phase):
        if phase == 0:
            @pl.when(it < steps // 2 - 2)
            def _():
                ag_own(2 * it + 4)
                ag_own(2 * it + 5)
        elif phase == 1:
            @pl.when(it < steps // 2 - 1)
            def _():
                ag_forward(2 * it + 2)
                ag_forward(2 * it + 3)
        else:
            @pl.when((it >= 1) & (it < steps // 2))
            def _():
                ag_relay(2 * it)

            @pl.when(it < steps // 2)
            def _():
                ag_relay(2 * it + 1)

    @pl.loop(0, steps + LEAD + FINAL_LAG)
    def _(it):
        @pl.when(it >= RING)
        def _():
            sent(it - RING)

        @pl.when(it < steps)
        def _():
            ag_ready(it)

        gather(it, 0)
        for p in range(group):
            ahead = p + CACHE_SLOTS - 1
            nxt = it + ahead // group

            @pl.when(valid(nxt, ahead % group))
            def _():
                c_load(nxt, ahead % group).start()

            @pl.when(valid(it, p))
            def _():
                attend(it, p, (6, 7, 0, 2, 1, 3, 4, 5)[p])
                if p == PM:
                    lse_a[it % RING] = lse_acc[...].T[6:8]
                    pm_copy(it).start()
                    la_copy(it).start()
                elif p in (D0, D1):
                    d_copy(it, p - D0).start()
                elif p in (F0, F1):
                    f_copy(it, p - F0).start()
                elif p == PF:
                    f_copy(it, 2).start()
                if p == F1:
                    merge(it)
                    m_copy(it).start()
                    ml_copy(it).start()

            if p == D1:
                gather(it, 1)
            if p == F1:
                gather(it, 2)

        @pl.when(it < steps + LEAD)
        def _():
            rows = lse_acc[...].T
            for t in range(3):
                lse_b[it % RING, t] = rows[2 * t:2 * t + 2]
            for t in range(3):
                lb_copy(it, t).start()

        @pl.when(it >= LEAD + FINAL_LAG)
        def _():
            k = it - FINAL_LAG

            final(k)

    @pl.loop(steps + LEAD + FINAL_LAG - RING, steps + LEAD)
    def _(it):
        sent(it)

    for kind in range(7):
        wait_bytes(q_all.at[:, :, kind], ag_send.at[kind])


def solution(mesh):
    group = mesh.shape['dcp']

    def local_step(q_blk, cache_blk, len_blk):
        batch, own_heads, width = q_blk.shape
        pages, page_len = cache_blk.shape[1], cache_blk.shape[3]
        steps = batch // group
        heads = own_heads * group
        latent = width - ROPE_DIM
        bf16, f32 = jnp.bfloat16, jnp.float32
        dma = pltpu.SemaphoreType.DMA
        return pl.pallas_call(
            functools.partial(_kernel, (steps, group, heads, latent, pages, page_len)),
            out_shape=jax.ShapeDtypeStruct((steps, heads, latent), bf16),
            in_specs=[pl.BlockSpec(memory_space=pltpu.HBM)] * 3,
            out_specs=pl.BlockSpec(memory_space=pltpu.VMEM),
            scratch_shapes=[
                pltpu.SMEM((batch,), jnp.int32),
                pltpu.VMEM((own_heads, width, batch), bf16),
                pltpu.VMEM((steps, group + 1, group, own_heads, latent), bf16),
                pltpu.VMEM((CACHE_SLOTS, pages, width, page_len), bf16),
                pltpu.VMEM((RING, group, heads, latent), bf16),
                pltpu.VMEM((heads, 128), f32),
                pltpu.VMEM((RING, 2, heads), f32),
                pltpu.VMEM((RING, 3, 2, heads), f32),
                pltpu.VMEM((steps, 3, heads, latent), bf16),
                pltpu.VMEM((steps, 3, heads, latent), bf16),
                pltpu.VMEM((steps, 2, heads), f32),
                pltpu.VMEM((steps + LEAD, 3, 2, heads), f32),
                pltpu.VMEM((RING, heads, latent), f32),
                pltpu.VMEM((RING, 1, heads), f32),
                pltpu.VMEM((steps, heads, latent), f32),
                pltpu.VMEM((steps, 1, heads), f32),
                pltpu.VMEM((128, heads), f32),
                dma, dma((own_heads // Q_PART,)), dma((CACHE_SLOTS,)),
                dma((7,)), dma((AG_RING, 3)), dma((steps,)),
                *[dma((RING,))] * 6, *[dma((RX_RING,))] * 6,
            ],
            compiler_params=pltpu.CompilerParams(collective_id=0, has_side_effects=True, vmem_limit_bytes=VMEM_BYTES),
        )(pltpu.with_memory_space_constraint(len_blk, pltpu.HBM), jnp.transpose(q_blk, (1, 2, 0)), jnp.swapaxes(cache_blk, 3, 4))

    return jax.shard_map(local_step, mesh=mesh, in_specs=(P('dp', 'dcp', None), P('dp', None, 'dcp', None, None), P('dp')),
                         out_specs=P(('dp', 'dcp'), None, None), check_vma=False)
```
